16 devices in a mesh: data: 2 (over y, z), tensor: 8 (over x, core).
Axes of the slice: x: 4, y: 2, z: 1, core: 2. Of those that a mesh axis runs over, the one named last changes fastest.
The devices are a block of a 4x4x8 slice.
Arguments:
- token_ids: int32 [65536], P(('data', 'tensor')), parts along dimension 0
- emb_table: bfloat16 [50304, 512], P('tensor')
- norm_gain: bfloat16 [512], replicated
- w_up: bfloat16 [512, 2048], P(None, 'tensor')
- w_down: bfloat16 [2048, 512], P('tensor')
- grad_out: bfloat16 [65536, 512], P(('data', 'tensor')), parts along dimension 0
Outputs:
- output 1: bfloat16 [65536, 512], P(('data', 'tensor')), parts along dimension 0
- output 2: float32 [100608, 512], P(('data', 'tensor')), parts along dimension 0
- output 3: float32 [1024, 2048], P('data', 'tensor'), parts along dimension 0
- output 4: float32 [4096, 512], P(('data', 'tensor')), parts along dimension 0
There are 2 independent parts. The reference program is written for one: setup_inputs(seed, part) draws one part's arguments, and reference() takes and returns one part's arrays. A program takes and returns all parts, laid end to end along the dimension named above; an argument that names none is the same for every part.
All inputs are finite; a program needn't handle non-finite values.
Results may differ from the reference program's by a relative error of at most 0.00554922.
Values are sent between devices in bfloat16 or wider.
A program may use at most 768 MiB of HBM per device.

```python
import math
import jax
import jax.numpy as jnp
from jax import lax

VOCAB_SIZE = 50304
MODEL_DIM = 512
FFN_DIM = 2048
TOKENS = 32768
HOT_IDS = 64
EPS = 1e-6
ROW_BLOCK = math.gcd(TOKENS, 2048)
NUM_BLOCKS = TOKENS // ROW_BLOCK


def draw_ids(key):
    key_uni, key_table, key_pick, key_coin = jax.random.split(key, 4)
    uniform_ids = jax.random.randint(key_uni, (TOKENS,), 0, VOCAB_SIZE)
    hot_table = jax.random.randint(key_table, (HOT_IDS,), 0, VOCAB_SIZE)
    hot_ids = hot_table[jax.random.randint(key_pick, (TOKENS,), 0, HOT_IDS)]
    coin_flip = jax.random.randint(key_coin, (TOKENS,), 0, 2)
    token_ids = jnp.where(coin_flip == 0, uniform_ids, hot_ids)
    token_ids = token_ids.at[0].set(0).at[TOKENS - 1].set(VOCAB_SIZE - 1)
    return token_ids.astype(jnp.int32)


def setup_inputs(seed: int = 0, part: int = 0) -> dict:
    shared_key, part_root = jax.random.split(jax.random.key(seed))
    key_emb, key_gain, key_up, key_down = jax.random.split(shared_key, 4)
    key_ids, key_grad = jax.random.split(jax.random.fold_in(part_root, part))
    emb_table = jax.random.normal(key_emb, (VOCAB_SIZE, MODEL_DIM), jnp.float32)
    norm_gain = 1.0 + 0.4 * jax.random.normal(key_gain, (MODEL_DIM,), jnp.float32)
    w_up = jax.random.normal(key_up, (MODEL_DIM, FFN_DIM), jnp.float32) * MODEL_DIM ** -0.5
    w_down = jax.random.normal(key_down, (FFN_DIM, MODEL_DIM), jnp.float32) * FFN_DIM ** -0.5
    grad_out = jax.random.normal(key_grad, (TOKENS, MODEL_DIM), jnp.float32)
    return {
        'token_ids': draw_ids(key_ids),
        'emb_table': emb_table.astype(jnp.bfloat16),
        'norm_gain': norm_gain.astype(jnp.bfloat16),
        'w_up': w_up.astype(jnp.bfloat16),
        'w_down': w_down.astype(jnp.bfloat16),
        'grad_out': grad_out.astype(jnp.bfloat16),
    }


def rms_norm(x_rows, gain_f):
    inv_rms = lax.rsqrt(jnp.mean(x_rows * x_rows, axis=-1, keepdims=True) + EPS)
    return x_rows * inv_rms * gain_f


def gelu_tanh(values):
    return jax.nn.gelu(values, approximate=True)


def reference(token_ids, emb_table, norm_gain, w_up, w_down, grad_out):
    gain_f = norm_gain.astype(jnp.float32)
    x_rows = jnp.take(emb_table, token_ids, axis=0)
    x_blocks = x_rows.reshape(NUM_BLOCKS, ROW_BLOCK, MODEL_DIM)
    grad_blocks = grad_out.reshape(NUM_BLOCKS, ROW_BLOCK, MODEL_DIM)

    def block_step(acc_pair, block_in):
        acc_up, acc_down = acc_pair
        x_blk = block_in[0].astype(jnp.float32)
        grad_blk = block_in[1]
        normed_f, norm_back = jax.vjp(lambda x_in: rms_norm(x_in, gain_f), x_blk)
        normed = normed_f.astype(jnp.bfloat16)
        pre_act = jnp.dot(normed, w_up, preferred_element_type=jnp.float32).astype(jnp.bfloat16)
        act_f, gelu_back = jax.vjp(gelu_tanh, pre_act.astype(jnp.float32))
        hidden = act_f.astype(jnp.bfloat16)
        y_blk = jnp.dot(hidden, w_down, preferred_element_type=jnp.float32)
        out_blk = (x_blk + y_blk).astype(jnp.bfloat16)
        d_hidden = jnp.dot(grad_blk, w_down.T, preferred_element_type=jnp.float32)
        d_pre = gelu_back(d_hidden)[0].astype(jnp.bfloat16)
        acc_down = acc_down + jnp.dot(hidden.T, grad_blk, preferred_element_type=jnp.float32)
        acc_up = acc_up + jnp.dot(normed.T, d_pre, preferred_element_type=jnp.float32)
        d_norm = jnp.dot(d_pre, w_up.T, preferred_element_type=jnp.float32)
        dx_blk = (grad_blk.astype(jnp.float32) + norm_back(d_norm)[0]).astype(jnp.bfloat16)
        return (acc_up, acc_down), (out_blk, dx_blk)

    zero_acc = (jnp.zeros((MODEL_DIM, FFN_DIM), jnp.float32), jnp.zeros((FFN_DIM, MODEL_DIM), jnp.float32))
    grads, outs = lax.scan(block_step, zero_acc, (x_blocks, grad_blocks))
    out = outs[0].reshape(TOKENS, MODEL_DIM)
    d_x = outs[1].reshape(TOKENS, MODEL_DIM).astype(jnp.float32)
    d_emb = jax.ops.segment_sum(d_x, token_ids, num_segments=VOCAB_SIZE)
    return (out, d_emb, grads[0], grads[1])
```

```python
import functools

import jax
import jax.numpy as jnp
from jax import lax
from jax.experimental import pallas as pl
from jax.experimental.pallas import tpu as pltpu
from jax.sharding import PartitionSpec as P

EPS = 1e-6
F32 = jnp.float32
BF16 = jnp.bfloat16
I32 = jnp.int32
MESH = pl.DeviceIdType.MESH
LANES = 128
UNROLL = 16
PAGE = 1024
AXIS = 'tensor'


def group_barrier(n, me):
    sem = pltpu.get_barrier_semaphore()
    for k in range(1, n):
        pl.semaphore_signal(sem, inc=1, device_id={AXIS: lax.rem(me + k, n)}, device_id_type=MESH)
    pl.semaphore_wait(sem, n - 1)


def far_first(n):
    return sorted(range(1, n), key=lambda k: -min(k // 2, (n - k) // 2))


def blocks(count, size, many, one):
    total = count // size

    def body(b, carry):
        for u in range(many):
            one(pl.multiple_of((b * many + u) * size, size))
        return carry

    lax.fori_loop(0, total // many, body, 0)
    for b in range(total // many * many, total):
        one(b * size)


def split_rows(src, dst, dst_row, count):
    w = src.shape[-1] // LANES

    def one(r0):
        tile = src[pl.ds(r0, 16), :].astype(F32)
        for c in range(w):
            dst[pl.ds((dst_row + r0) * w + c, 16, stride=w), :] = tile[:, c * LANES:(c + 1) * LANES]

    blocks(count, 16, 4, one)


def join_rows(src, dst, dst_row, count):
    w = dst.shape[-1] // LANES

    def one(r0):
        parts = [src[pl.ds(r0 * w + c, 16, stride=w), :] for c in range(w)]
        dst[pl.ds(pl.multiple_of(dst_row + r0, 16), 16), :] = jnp.concatenate(parts, axis=1).astype(dst.dtype)

    blocks(count, 16, 4, one)


def pick_rows(src, dst, dst_row, count, w, index):
    def body(b, carry):
        vals = []
        for u in range(UNROLL):
            line = pl.multiple_of(index(b * UNROLL + u), w)
            vals.append(src[pl.ds(line, w), :])
        for u in range(UNROLL):
            dst[pl.ds(pl.multiple_of((dst_row + b * UNROLL + u) * w, w), w), :] = vals[u]
        return carry

    lax.fori_loop(0, count // UNROLL, body, 0)


def any_spec():
    return pl.BlockSpec(memory_space=pl.ANY)


def smem_spec():
    return pl.BlockSpec(memory_space=pltpu.SMEM)


def vmem_spec():
    return pl.BlockSpec(memory_space=pltpu.VMEM)


DMA = pltpu.SemaphoreType.DMA


K0 = 0.7978845608028654
K1 = 0.044715


def dot_nn(a, b):
    return lax.dot_general(a, b, (((1,), (0,)), ((), ())), preferred_element_type=F32)


def dot_nt(a, b):
    return lax.dot_general(a, b, (((1,), (1,)), ((), ())), preferred_element_type=F32)


def gelu_pair(u, dh):
    u2 = u * u
    t = jnp.tanh(u * (K0 + (K0 * K1) * u2))
    s = 0.5 + 0.5 * t
    h = u * s
    slope = s + h * (1.0 - s) * (2.0 * K0 + (6.0 * K0 * K1) * u2)
    return h.astype(BF16), (dh * slope).astype(BF16)


def mlp_kernel(n, tc, x_hbm, g_ref, w1_ref, w2_ref, do_hbm, out_hbm, dx_hbm, dw1_hbm, dw2_hbm,
               x_v, do_v, n_v, nt_v, dot_v, y_v, dn_v, h_v, du_v, dw1_v, dw2_v, in_sem, out_sem, dw_sem):
    t_all, d = x_v.shape
    nc = t_all // tc
    rows = lambda c: pl.ds(pl.multiple_of(c * tc, tc), tc)
    for c in range(nc):
        pltpu.make_async_copy(x_hbm.at[pl.ds(c * tc, tc)], x_v.at[pl.ds(c * tc, tc)], in_sem.at[0, c]).start()
        pltpu.make_async_copy(do_hbm.at[pl.ds(c * tc, tc)], do_v.at[pl.ds(c * tc, tc)], in_sem.at[1, c]).start()
    gain = g_ref[...].astype(F32)

    def prep(c, carry):
        r = rows(c)
        pltpu.make_async_copy(x_hbm.at[r], x_v.at[r], in_sem.at[0, c]).wait()
        pltpu.make_async_copy(do_hbm.at[r], do_v.at[r], in_sem.at[1, c]).wait()
        xf = x_v[r, :].astype(F32)
        inv = lax.rsqrt(jnp.mean(xf * xf, axis=-1, keepdims=True) + EPS)
        nb = (xf * inv * gain).astype(BF16)
        n_v[r, :] = nb
        nt_v[:, r] = nb.T
        dot_v[:, r] = do_v[r, :].T
        y_v[r, :] = jnp.zeros((tc, d), F32)
        dn_v[r, :] = jnp.zeros((tc, d), F32)
        return carry

    lax.fori_loop(0, nc, prep, 0)

    def first(j, c, slot):
        r = rows(c)
        u = dot_nn(n_v[r, :], w1_ref[j]).astype(BF16).astype(F32)
        dh = dot_nt(do_v[r, :], w2_ref[j])
        h, du = gelu_pair(u, dh)
        h_v[slot] = h
        du_v[slot] = du

    def second(j, c, slot):
        r = rows(c)
        h = h_v[slot]
        du = du_v[slot]
        y_v[r, :] += dot_nn(h, w2_ref[j])
        dn_v[r, :] += dot_nt(du, w1_ref[j])
        b = lax.rem(j, 2)
        dw1_v[b] += dot_nn(nt_v[:, r], du)
        dw2_v[b] += dot_nn(dot_v[:, r], h)

    steps = n * nc
    first(0, 0, 0)

    def body(i, carry):
        j, c = lax.div(i, nc), lax.rem(i, nc)
        b = lax.rem(j, 2)

        @pl.when(c == 0)
        def _():
            @pl.when(j >= 2)
            def _():
                pltpu.make_async_copy(dw1_v.at[b], dw1_hbm.at[j - 2], dw_sem.at[0, b]).wait()
                pltpu.make_async_copy(dw2_v.at[b], dw2_hbm.at[j - 2], dw_sem.at[1, b]).wait()
            dw1_v[b] = jnp.zeros(dw1_v.shape[1:], F32)
            dw2_v[b] = jnp.zeros(dw2_v.shape[1:], F32)

        nxt = lax.rem(i + 1, steps)
        slot = lax.rem(i, 2)
        second(j, c, slot)
        first(lax.div(nxt, nc), lax.rem(nxt, nc), 1 - slot)

        @pl.when(c == nc - 1)
        def _():
            pltpu.make_async_copy(dw1_v.at[b], dw1_hbm.at[j], dw_sem.at[0, b]).start()
            pltpu.make_async_copy(dw2_v.at[b], dw2_hbm.at[j], dw_sem.at[1, b]).start()
        return carry

    lax.fori_loop(0, steps, body, 0)

    def tail(c, carry):
        r = rows(c)
        xf = x_v[r, :].astype(F32)
        inv = lax.rsqrt(jnp.mean(xf * xf, axis=-1, keepdims=True) + EPS)
        w = dn_v[r, :] * gain
        proj = jnp.mean(xf * w, axis=-1, keepdims=True) * (inv * inv * inv)
        dx = do_v[r, :].astype(F32) + (w * inv - xf * proj)
        do_v[r, :] = dx.astype(BF16)
        x_v[r, :] = (xf + y_v[r, :]).astype(BF16)
        pltpu.make_async_copy(do_v.at[r], dx_hbm.at[r], out_sem.at[1]).start()
        pltpu.make_async_copy(x_v.at[r], out_hbm.at[r], out_sem.at[0]).start()
        return carry

    lax.fori_loop(0, nc, tail, 0)
    for b in range(2):
        j = n - 2 + b
        pltpu.make_async_copy(dw1_v.at[j % 2], dw1_hbm.at[j], dw_sem.at[0, j % 2]).wait()
        pltpu.make_async_copy(dw2_v.at[j % 2], dw2_hbm.at[j], dw_sem.at[1, j % 2]).wait()
    pltpu.make_async_copy(do_v, dx_hbm, out_sem.at[1]).wait()
    pltpu.make_async_copy(x_v, out_hbm, out_sem.at[0]).wait()


def mlp(x, g, w1s, w2s, dout, tc=1024):
    t, d = x.shape
    n, _, fs = w1s.shape
    nc = t // tc
    any_ = pl.BlockSpec(memory_space=pl.ANY)
    vm = pl.BlockSpec(memory_space=pltpu.VMEM)
    return pl.pallas_call(
        functools.partial(mlp_kernel, n, tc),
        out_shape=(
            jax.ShapeDtypeStruct((t, d), BF16),
            jax.ShapeDtypeStruct((t, d), BF16),
            jax.ShapeDtypeStruct((n, d, fs), F32),
            jax.ShapeDtypeStruct((n, d, fs), F32),
        ),
        in_specs=[any_, vm, vm, vm, any_],
        out_specs=[any_] * 4,
        scratch_shapes=[
            pltpu.VMEM((t, d), BF16), pltpu.VMEM((t, d), BF16), pltpu.VMEM((t, d), BF16),
            pltpu.VMEM((d, t), BF16), pltpu.VMEM((d, t), BF16),
            pltpu.VMEM((t, d), F32), pltpu.VMEM((t, d), F32),
            pltpu.VMEM((2, tc, fs), BF16), pltpu.VMEM((2, tc, fs), BF16),
            pltpu.VMEM((2, d, fs), F32), pltpu.VMEM((2, d, fs), F32),
            pltpu.SemaphoreType.DMA((2, nc)), pltpu.SemaphoreType.DMA((2,)), pltpu.SemaphoreType.DMA((2, 2)),
        ],
        compiler_params=pltpu.CompilerParams(vmem_limit_bytes=63 << 20),
        cost_estimate=pl.CostEstimate(flops=12 * t * d * n * fs, bytes_accessed=40 << 20, transcendentals=t * n * fs),
    )(x, g.reshape(1, d), w1s, w2s, dout)


def share_kernel(n, others, pack, need, lists, most, got, relay, ss, rs, ns, nr, own_sem, xs_sem, xr_sem):
    me = lax.axis_index(AXIS)
    pl_len = pack.shape[0]
    here = pl.ds(pl.multiple_of(me * pl_len, PAGE), pl_len)
    own = pltpu.make_async_copy(pack, lists.at[here], own_sem)
    own.start()
    hops = []
    for name, size in others:
        reach = 1
        while reach < size:
            hops.append((name, size, reach))
            reach *= 2
    sem = pltpu.get_barrier_semaphore()
    for k in range(1, n):
        pl.semaphore_signal(sem, inc=1, device_id={AXIS: lax.rem(me + k, n)}, device_id_type=MESH)
    for name, size, reach in hops:
        at = lax.axis_index(name)
        pl.semaphore_signal(sem, inc=1, device_id={name: lax.rem(at + size - reach, size)}, device_id_type=MESH)
    pl.semaphore_wait(sem, n - 1 + len(hops))

    def list_copy(k):
        return pltpu.make_async_remote_copy(pack, lists.at[here], ss.at[k], rs.at[k],
                                            device_id={AXIS: lax.rem(me + k, n)}, device_id_type=MESH)

    def need_copy(k):
        return pltpu.make_async_remote_copy(need, got.at[k], ns.at[k], nr.at[k],
                                            device_id={AXIS: lax.rem(me + k, n)}, device_id_type=MESH)

    for k in far_first(n):
        need_copy(k).start()
        list_copy(k).start()
    top = need[...]
    for k in range(1, n):
        need_copy(k).wait_recv()
        top = jnp.maximum(top, got[k])
    for i, (name, size, reach) in enumerate(hops):
        relay[2 * i] = top
        at = lax.axis_index(name)
        hop = pltpu.make_async_remote_copy(relay.at[2 * i], relay.at[2 * i + 1], xs_sem.at[i], xr_sem.at[i],
                                           device_id={name: lax.rem(at + reach, size)}, device_id_type=MESH)
        hop.start()
        hop.wait()
        top = jnp.maximum(top, relay[2 * i + 1])
    most[...] = top
    for k in range(1, n):
        need_copy(k).wait_send()
        list_copy(k).wait()
    own.wait()


def share(n, others, pack, need):
    steps = max(1, sum((size - 1).bit_length() for _, size in others))
    tile = (8, LANES)
    return pl.pallas_call(
        functools.partial(share_kernel, n, others),
        out_shape=(jax.ShapeDtypeStruct((n * pack.shape[0],), I32), jax.ShapeDtypeStruct(tile, I32)),
        in_specs=[any_spec(), vmem_spec()],
        out_specs=(any_spec(), vmem_spec()),
        scratch_shapes=[pltpu.VMEM((n,) + tile, I32), pltpu.VMEM((2 * steps,) + tile, I32),
                        DMA((n,)), DMA((n,)), DMA((n,)), DMA((n,)), DMA, DMA((steps,)), DMA((steps,))],
        compiler_params=pltpu.CompilerParams(collective_id=1, has_side_effects=True),
        name='share_lists',
    )(pack, need)


def serve_kernel(n, c1, c2, rnd_ref, who_ref, ls, table, sent, e_st, ef, g, e_sem):
    me, rnd = who_ref[0], rnd_ref[0]
    vocab, d = e_st.shape
    w = d // LANES
    pl_len = ls.shape[0] // n
    head = pl_len - PAGE
    last = head - c1 - c2
    parts = e_sem.shape[0]
    step = vocab // parts

    def load(i):
        return pltpu.make_async_copy(table.at[pl.ds(i * step, step)], e_st.at[pl.ds(i * step, step)], e_sem.at[i])

    for i in range(parts):
        load(i).start()
    for i in range(parts):
        load(i).wait()
        split_rows(e_st.at[pl.ds(i * step, step)], ef, i * step, step)

    def source(q, carry):
        at1 = q * pl_len + jnp.minimum(ls[q * pl_len + head + me] + rnd * c1, last)
        at2 = q * pl_len + jnp.minimum(ls[q * pl_len + head + 16 + me] + rnd * c2, last)
        pick_rows(ef, g, 0, c1, w, lambda j: ls[at1 + j])
        pick_rows(ef, g, c1, c2, w, lambda j: ls[at2 + j])
        join_rows(g, sent.at[q], 0, c1 + c2)
        return carry

    lax.fori_loop(0, n, source, 0)


def serve(n, c1, c2, rnd, who, lists, table):
    vocab, d = table.shape
    w = d // LANES
    c = c1 + c2
    parts = 3 if vocab % 48 == 0 else 1
    return pl.pallas_call(
        functools.partial(serve_kernel, n, c1, c2),
        out_shape=jax.ShapeDtypeStruct((n, c, d), BF16),
        in_specs=[smem_spec(), smem_spec(), smem_spec(), any_spec()],
        out_specs=vmem_spec(),
        scratch_shapes=[pltpu.VMEM((vocab, d), BF16), pltpu.VMEM((vocab * w, LANES), F32),
                        pltpu.VMEM((c * w, LANES), F32), DMA((parts,))],
        compiler_params=pltpu.CompilerParams(vmem_limit_bytes=48 << 20),
        name='serve_rows',
    )(rnd, who, lists, table)


def swap_kernel(n, arrays, *refs):
    srcs, dsts, (ss, rs) = refs[:arrays], refs[arrays:2 * arrays], refs[2 * arrays:]
    me = lax.axis_index(AXIS)
    group_barrier(n, me)

    def copy(a, k):
        p = lax.rem(me + k, n)
        return pltpu.make_async_remote_copy(srcs[a].at[p], dsts[a].at[me], ss.at[a, k], rs.at[a, k],
                                            device_id={AXIS: p}, device_id_type=MESH)

    for k in far_first(n):
        for a in range(arrays):
            copy(a, k).start()
    for k in far_first(n):
        for a in range(arrays):
            copy(a, k).wait()


def swap(n, cid, name, *arrays):
    m = len(arrays)
    return pl.pallas_call(
        functools.partial(swap_kernel, n, m),
        out_shape=tuple(jax.ShapeDtypeStruct(a.shape, a.dtype) for a in arrays),
        in_specs=[any_spec()] * m,
        out_specs=(any_spec(),) * m,
        scratch_shapes=[DMA((m, n)), DMA((m, n))],
        compiler_params=pltpu.CompilerParams(collective_id=cid, has_side_effects=True),
        name=name,
    )(*arrays)


def expand_kernel(n, c, again, *refs):
    if again:
        rnd_ref, who_ref, toks, lines, sent, got, x_prev, x_out, rb, rf, xg, in_sem, x_sem = refs
    else:
        rnd_ref, who_ref, toks, lines, sent, got, x_out, rb, rf, xg, in_sem = refs
    me, rnd = who_ref[0], rnd_ref[0]
    t, d = x_out.shape
    w = d // LANES
    own = pltpu.make_async_copy(sent.at[me], rb.at[me], in_sem.at[me])
    own.start()
    if again:
        prev = pltpu.make_async_copy(x_prev, x_out, x_sem)
        prev.start()

    def load(q):
        return pltpu.make_async_copy(got.at[q], rb.at[q], in_sem.at[q])

    for k in range(n):
        @pl.when(k != me)
        def _():
            load(k).start()
    if again:
        prev.wait()
        split_rows(x_out, xg, 0, t)

    def source(q, carry):
        load(q).wait()
        split_rows(rb.at[q], rf, q * c, c)
        return carry

    lax.fori_loop(0, n, source, 0)
    low = rnd * (n * c * w)
    high = n * c * w

    def body(b, carry):
        vals, dst = [], []
        for u in range(UNROLL):
            i = b * UNROLL + u
            line = lines[i] - low
            here = (line >= 0) & (line < high)
            dst.append(pl.multiple_of(jnp.where(here, toks[i], t * w), w))
            vals.append(rf[pl.ds(pl.multiple_of(jnp.where(here, line, 0), w), w), :])
        for u in range(UNROLL):
            xg[pl.ds(dst[u], w), :] = vals[u]
        return carry

    lax.fori_loop(0, t // UNROLL, body, 0)
    join_rows(xg, x_out, 0, t)


def expand(n, rnd, who, toks, lines, sent, got, x_prev=None):
    again = x_prev is not None
    t = toks.shape[0]
    _, c, d = sent.shape
    w = d // LANES
    return pl.pallas_call(
        functools.partial(expand_kernel, n, c, again),
        out_shape=jax.ShapeDtypeStruct((t, d), BF16),
        in_specs=[smem_spec()] * 4 + [any_spec()] * (3 if again else 2),
        out_specs=vmem_spec(),
        scratch_shapes=[pltpu.VMEM((n, c, d), BF16), pltpu.VMEM((n * c * w, LANES), F32),
                        pltpu.VMEM((t * w + 8, LANES), F32), DMA((n,))] + ([DMA] if again else []),
        compiler_params=pltpu.CompilerParams(vmem_limit_bytes=48 << 20),
        name='expand_more' if again else 'expand_rows',
    )(rnd, who, toks, lines, sent, got, *((x_prev,) if again else ()))


def collect_kernel(n, c1, c2, vocab, rnd_ref, pack, toks, ids, dx_hbm, one, many, dx_v, dxf, g, col, in_sem):
    rnd = rnd_ref[0]
    t, d = dx_v.shape
    w = d // LANES
    parts = in_sem.shape[0]
    step = t // parts
    head = pack.shape[0] - PAGE
    last = head - c1 - c2

    def load(i):
        rows = pl.ds(pl.multiple_of(i * step, step), step)
        return pltpu.make_async_copy(dx_hbm.at[rows], dx_v.at[rows], in_sem.at[i])

    for i in range(parts):
        load(i).start()

    def name_rows(q, carry):
        at = jnp.minimum(pack[head + 16 + q] + rnd * c2, last)
        for j in range(c2):
            col[pl.ds(q * c2 + j, 1), :] = jnp.full((1, LANES), pack[at + j] + q * (vocab * w), I32)
        return carry

    lax.fori_loop(0, n, name_rows, 0)
    many[...] = jnp.zeros(many.shape, F32)
    names = col[:, :1]

    def sum_many(i, carry):
        load(i).wait()
        hot = jnp.where(names == ids[i] * w, 1.0, 0.0).astype(BF16)
        rows = pl.ds(pl.multiple_of(i * step, step), step)
        many[...] += lax.dot_general(hot, dx_v[rows, :], (((1,), (0,)), ((), ())), preferred_element_type=F32)
        split_rows(dx_v.at[rows], dxf, i * step, step)
        return carry

    lax.fori_loop(0, parts, sum_many, 0)

    def owner(q, carry):
        at = jnp.minimum(pack[head + q] + rnd * c1, last)
        pick_rows(dxf, g, 0, c1, w, lambda j: toks[at + j])
        join_rows(g, one.at[q], 0, c1)
        return carry

    lax.fori_loop(0, n, owner, 0)


def collect(n, c1, c2, vocab, rnd, pack, toks, ids, dx):
    t, d = dx.shape
    w = d // LANES
    parts = ids.shape[0]
    one, many = pl.pallas_call(
        functools.partial(collect_kernel, n, c1, c2, vocab),
        out_shape=(jax.ShapeDtypeStruct((n, c1, d), BF16), jax.ShapeDtypeStruct((n * c2, d), F32)),
        in_specs=[smem_spec(), smem_spec(), smem_spec(), vmem_spec(), any_spec()],
        out_specs=(vmem_spec(), vmem_spec()),
        scratch_shapes=[pltpu.VMEM((t, d), BF16), pltpu.VMEM((t * w, LANES), F32), pltpu.VMEM((c1 * w, LANES), F32),
                        pltpu.VMEM((n * c2, LANES), I32), DMA((parts,))],
        compiler_params=pltpu.CompilerParams(vmem_limit_bytes=48 << 20),
        name='collect_rows',
    )(rnd, pack, toks, ids, dx)
    return one, many.reshape(n, c2, d)


def place_kernel(n, c1, c2, again, *refs):
    if again:
        rnd_ref, who_ref, ls, one_own, many_own, one, many, _, out, acc, o_v, m_v, f_v, st, in_sem, out_sem = refs
    else:
        rnd_ref, who_ref, ls, one_own, many_own, one, many, out, acc, o_v, m_v, f_v, st, in_sem, out_sem = refs
    me, rnd = who_ref[0], rnd_ref[0]
    vocab, d = out.shape
    w = d // LANES
    pl_len = ls.shape[0] // n
    head = pl_len - PAGE

    def load(q):
        return (pltpu.make_async_copy(one.at[q], o_v.at[q], in_sem.at[0, q]),
                pltpu.make_async_copy(many.at[q], m_v.at[q], in_sem.at[1, q]))

    pltpu.make_async_copy(one_own.at[me], o_v.at[me], in_sem.at[0, me]).start()
    pltpu.make_async_copy(many_own.at[me], m_v.at[me], in_sem.at[1, me]).start()
    for k in range(n):
        @pl.when(k != me)
        def _():
            for part in load(k):
                part.start()
    blk = st.shape[1]

    def span(i):
        return pl.ds(pl.multiple_of(i * blk, blk), blk)

    def split8(src, row):
        def one8(r0):
            for k in range(w):
                acc[pl.ds((row + r0) * w + k, 8, stride=w), :] = src[pl.ds(r0, 8), pl.ds(k * LANES, LANES)]
        blocks(blk, 8, 8, one8)

    if again:
        def bring(i, carry):
            pltpu.make_async_copy(out.at[span(i)], st.at[0], out_sem.at[0]).start()
            pltpu.make_async_copy(out.at[span(i)], st.at[0], out_sem.at[0]).wait()
            split8(st.at[0], i * blk)
            return carry

        lax.fori_loop(0, vocab // blk, bring, 0)
    else:
        zero = jnp.zeros((16 * w, LANES), F32)

        def clear(r0):
            acc[pl.ds(r0 * w, 16 * w), :] = zero

        blocks(vocab, 16, 4, clear)
    dump = vocab * w

    def add(count, at, row0):
        def body(b, carry):
            lines, sums = [], []
            for u in range(UNROLL):
                j = b * UNROLL + u
                line = pl.multiple_of(jnp.where(j < count, ls[at + j], dump), w)
                lines.append(line)
                src = f_v[pl.ds(pl.multiple_of((row0 + j) * w, w), w), :]
                sums.append(acc[pl.ds(line, w), :] + src)
            for u in range(UNROLL):
                acc[pl.ds(lines[u], w), :] = sums[u]
            return carry

        lax.fori_loop(0, lax.div(count + UNROLL - 1, UNROLL), body, 0)

    def source(q, carry):
        for part in load(q):
            part.wait()
        at = q * pl_len + head
        split_rows(o_v.at[q], f_v, 0, c1)
        split_rows(m_v.at[q], f_v, c1, c2)
        b1, b2 = ls[at + me] + rnd * c1, ls[at + 16 + me] + rnd * c2
        e1, e2 = ls[at + me + 1], ls[at + 16 + me + 1]
        add(jnp.clip(e1 - b1, 0, c1), q * pl_len + b1, 0)
        add(jnp.clip(e2 - b2, 0, c2), q * pl_len + b2, c1)
        return carry

    lax.fori_loop(0, n, source, 0)

    def emit(i, carry):
        slot = lax.rem(i, 2)

        @pl.when(i >= 2)
        def _():
            pltpu.make_async_copy(st.at[slot], out.at[span(i - 2)], out_sem.at[slot]).wait()

        def one8(r0):
            for k in range(w):
                st[slot, pl.ds(r0, 8), pl.ds(k * LANES, LANES)] = acc[pl.ds((i * blk + r0) * w + k, 8, stride=w), :]

        blocks(blk, 8, 8, one8)
        pltpu.make_async_copy(st.at[slot], out.at[span(i)], out_sem.at[slot]).start()
        return carry

    total = vocab // blk
    lax.fori_loop(0, total, emit, 0)
    for i in range(max(0, total - 2), total):
        pltpu.make_async_copy(st.at[i % 2], out.at[span(i)], out_sem.at[i % 2]).wait()


def place(n, c1, c2, vocab, rnd, who, lists, one_own, many_own, one, many, prev=None):
    again = prev is not None
    d = one.shape[-1]
    w = d // LANES
    blk = next(b for b in range(1024, 0, -8) if vocab % b == 0)
    return pl.pallas_call(
        functools.partial(place_kernel, n, c1, c2, again),
        out_shape=jax.ShapeDtypeStruct((vocab, d), F32),
        in_specs=[smem_spec()] * 3 + [any_spec()] * (5 if again else 4),
        out_specs=any_spec(),
        scratch_shapes=[
            pltpu.VMEM((vocab * w + 8, LANES), F32), pltpu.VMEM((n, c1, d), BF16), pltpu.VMEM((n, c2, d), F32),
            pltpu.VMEM(((c1 + c2) * w, LANES), F32), pltpu.VMEM((2, blk, d), F32), DMA((2, n)), DMA((2,)),
        ],
        input_output_aliases={7: 0} if again else {},
        compiler_params=pltpu.CompilerParams(vmem_limit_bytes=48 << 20),
        name='place_more' if again else 'place_rows',
    )(rnd, who, lists, one_own, many_own, one, many, *((prev,) if again else ()))


def route(n, vocab, w, c1, c2, ids):
    t = ids.shape[0]
    c = c1 + c2
    s, p = lax.sort((ids, lax.iota(I32, t)), num_keys=1)
    edge = jnp.full((1,), -1, I32)
    first = s != jnp.concatenate([edge, s[:-1]])
    last = s != jnp.concatenate([s[1:], edge])
    lone = first & last
    lead = first & ~last
    lone_i, lead_i = lone.astype(I32), lead.astype(I32)
    bounds = lax.iota(I32, n + 1) * vocab
    below = s[None, :] < bounds[:, None]
    base1 = jnp.sum(jnp.where(below, lone_i[None, :], 0), axis=1)
    base2 = jnp.sum(jnp.where(below, lead_i[None, :], 0), axis=1)
    owner = n - jnp.sum(below[1:].astype(I32), axis=0)
    mine = owner[None, :] == lax.iota(I32, n)[:, None]
    start1 = jnp.sum(jnp.where(mine, base1[:n, None], 0), axis=0)
    start2 = jnp.sum(jnp.where(mine, base2[:n, None], 0), axis=0)
    r1 = jnp.cumsum(lone_i) - lone_i - start1
    r2 = jnp.cumsum(lead_i) - 1 - start2
    rnd1, rnd2 = r1 // c1, r2 // c2
    slot = jnp.where(lone, rnd1 * (n * c) + owner * c + r1 - rnd1 * c1, rnd2 * (n * c) + owner * c + c1 + r2 - rnd2 * c2)
    kind = jnp.where(lone, 0, jnp.where(lead, 1, 2)) * t + lax.iota(I32, t)
    _, line, tok = lax.sort((kind, (s - owner * vocab) * w, p * w), num_keys=1)
    n1 = base1[n]
    room = -(-(t + c1 + c2) // PAGE) * PAGE
    spare = jnp.zeros((16 - n - 1,), I32)
    heads = jnp.concatenate([base1, spare, n1 + base2, spare])
    fill = jnp.zeros((room - t,), I32)
    heads = jnp.concatenate([heads, jnp.zeros((PAGE - heads.shape[0],), I32)])
    pack = jnp.concatenate([line, fill, heads])
    lone_tok = jnp.concatenate([tok, fill])
    per1 = jnp.max(base1[1:] - base1[:-1])
    per2 = jnp.max(base2[1:] - base2[:-1])
    rounds = jnp.maximum((per1 + c1 - 1) // c1, (per2 + c2 - 1) // c2)
    return pack, lone_tok, p * w, slot * w, rounds


def solution(mesh):
    n = mesh.shape[AXIS]
    axes = tuple(mesh.axis_names)
    others = tuple((name, mesh.shape[name]) for name in axes if name != AXIS)
    tok_spec = P(axes)
    row_spec = P(axes, None)

    def local_step(token_ids, emb_shard, norm_gain, w_up_l, w_down_l, grad_out):
        vocab, d = emb_shard.shape
        t = token_ids.shape[0]
        w = d // LANES
        c1 = -(-(t * 5 // (8 * n)) // 16) * 16
        c2 = -(-(t // 128) // 16) * 16
        who = lax.axis_index(AXIS)[None].astype(I32)
        w_up = lax.all_gather(w_up_l, AXIS)
        w_down = lax.all_gather(w_down_l, AXIS)
        pack, lone_tok, toks, lines, rounds = route(n, vocab, w, c1, c2, token_ids)
        lists, most = share(n, others, pack, jnp.full((8, LANES), rounds, I32))
        rounds = most[0, 0]
        none = jnp.zeros((1,), I32)

        def rows_of(rnd):
            sent = serve(n, c1, c2, rnd, who, lists, emb_shard)
            return sent, swap(n, 2, 'swap_rows', sent)[0]

        def more_rows(carry):
            r, x_now = carry
            return r + 1, expand(n, r[None], who, toks, lines, *rows_of(r[None]), x_now)

        x = expand(n, none, who, toks, lines, *rows_of(none))
        _, x = lax.while_loop(lambda carry: carry[0] < rounds, more_rows, (jnp.ones((), I32), x))
        out, dx, dw1, dw2t = mlp(x, norm_gain, w_up, w_down, grad_out)
        dw = lax.psum_scatter(jnp.concatenate([dw1, dw2t], axis=1), AXIS, scatter_dimension=0)
        ids_c = token_ids.reshape(-1, 1, t // 8)

        def sums_of(rnd):
            one, many = collect(n, c1, c2, vocab, rnd, pack, lone_tok, ids_c, dx)
            return (one, many) + swap(n, 3, 'swap_sums', one, many)

        def more_sums(carry):
            r, now = carry
            return r + 1, place(n, c1, c2, vocab, r[None], who, lists, *sums_of(r[None]), now)

        d_emb = place(n, c1, c2, vocab, none, who, lists, *sums_of(none))
        _, d_emb = lax.while_loop(lambda carry: carry[0] < rounds, more_sums, (jnp.ones((), I32), d_emb))
        return out, d_emb, dw[:d], dw[d:].T

    return jax.shard_map(
        local_step,
        mesh=mesh,
        in_specs=(tok_spec, P(AXIS, None), P(None), P(None, AXIS), P(AXIS, None), row_spec),
        out_specs=(row_spec, row_spec, P(axes[0], AXIS), row_spec),
        check_vma=False,
    )
```

```python
import functools

import jax
import jax.numpy as jnp
from jax import lax
from jax.experimental import pallas as pl
from jax.experimental.pallas import tpu as pltpu
from jax.sharding import PartitionSpec as P

EPS = 1e-6
F32 = jnp.float32
BF16 = jnp.bfloat16
I32 = jnp.int32
MESH = pl.DeviceIdType.MESH
LANES = 128
UNROLL = 16
PAGE = 1024
AXIS = 'tensor'


def group_barrier(n, me, wait=True):
    sem = pltpu.get_barrier_semaphore()
    for k in range(1, n):
        pl.semaphore_signal(sem, inc=1, device_id={AXIS: lax.rem(me + k, n)}, device_id_type=MESH)
    if wait:
        pl.semaphore_wait(sem, n - 1)


def far_first(n):
    return sorted(range(1, n), key=lambda k: -min(k // 2, (n - k) // 2))


def blocks(count, size, many, one):
    total = count // size

    def body(b, carry):
        for u in range(many):
            one(pl.multiple_of((b * many + u) * size, size))
        return carry

    lax.fori_loop(0, total // many, body, 0)
    for b in range(total // many * many, total):
        one(b * size)


def split_rows(src, dst, dst_row, count):
    w = src.shape[-1] // LANES

    def one(r0):
        tile = src[pl.ds(r0, 16), :].astype(F32)
        for c in range(w):
            dst[pl.ds((dst_row + r0) * w + c, 16, stride=w), :] = tile[:, c * LANES:(c + 1) * LANES]

    blocks(count, 16, 4, one)


def join_rows(src, dst, dst_row, count):
    w = dst.shape[-1] // LANES

    def one(r0):
        parts = [src[pl.ds(r0 * w + c, 16, stride=w), :] for c in range(w)]
        dst[pl.ds(pl.multiple_of(dst_row + r0, 16), 16), :] = jnp.concatenate(parts, axis=1).astype(dst.dtype)

    blocks(count, 16, 4, one)


def pick_rows(src, dst, dst_row, count, w, index):
    def body(b, carry):
        vals = []
        for u in range(UNROLL):
            line = pl.multiple_of(index(b * UNROLL + u), w)
            vals.append(src[pl.ds(line, w), :])
        for u in range(UNROLL):
            dst[pl.ds(pl.multiple_of((dst_row + b * UNROLL + u) * w, w), w), :] = vals[u]
        return carry

    lax.fori_loop(0, count // UNROLL, body, 0)


def any_spec():
    return pl.BlockSpec(memory_space=pltpu.HBM)


def smem_spec():
    return pl.BlockSpec(memory_space=pltpu.SMEM)


def vmem_spec():
    return pl.BlockSpec(memory_space=pltpu.VMEM)


DMA = pltpu.SemaphoreType.DMA


K0 = 0.7978845608028654
K1 = 0.044715


def dot_nn(a, b):
    return lax.dot_general(a, b, (((1,), (0,)), ((), ())), preferred_element_type=F32)


def dot_nt(a, b):
    return lax.dot_general(a, b, (((1,), (1,)), ((), ())), preferred_element_type=F32)


def gelu_pair(u, dh):
    u2 = u * u
    t = jnp.tanh(u * (K0 + (K0 * K1) * u2))
    s = 0.5 + 0.5 * t
    h = u * s
    slope = s + h * (1.0 - s) * (2.0 * K0 + (6.0 * K0 * K1) * u2)
    return h.astype(BF16), (dh * slope).astype(BF16)


def mlp_kernel(n, tc, x_hbm, g_ref, w1_hbm, w2_hbm, do_hbm, dh_hbm, dot_hbm, out_hbm, dx_hbm, dw1_hbm, dw2_hbm,
               x_v, do_v, n_v, nt_v, dot_v, y_v, dn_v, w1_ref, w2_ref, h_a, h_b, du_a, du_b, dh_a, dh_b, part, mate, ours, theirs,
               in_sem, w_sem, dh_sem, out_sem, dw_sem, ms, mr, cs, cr):
    me = lax.axis_index(AXIS)
    core, chip = lax.rem(me, 2), lax.div(me, 2)
    chips = n // 2
    far = sorted(range(1, chips), key=lambda k: -min(k, chips - k)) + [0]
    t_all, d = x_v.shape
    nc = t_all // tc
    rows = lambda c: pl.ds(pl.multiple_of(c * tc, tc), tc)
    mate_id = {AXIS: me + 1 - 2 * core}

    def load(c):
        r = rows(c)
        return pltpu.make_async_copy(x_hbm.at[r], x_v.at[r], in_sem.at[c])

    for c in range(nc):
        load(c).start()
    weights = (pltpu.make_async_copy(w1_hbm, w1_ref, w_sem.at[0]), pltpu.make_async_copy(w2_hbm, w2_ref, w_sem.at[1]),
               pltpu.make_async_copy(dot_hbm, dot_v, w_sem.at[2]))
    for cp in weights:
        cp.start()
    group_barrier(n, me, wait=False)
    late = pltpu.make_async_copy(do_hbm, do_v, w_sem.at[3])
    late.start()

    def owner_chip(q):
        off = sum(jnp.where(q == i, k, 0) for i, k in enumerate(far))
        return lax.rem(chip + off, chips)

    def block_of(jj):
        half = lax.rem(jj, 2)
        return 2 * owner_chip(lax.div(jj, 2)) + jnp.where(half == 0, 1 - core, core)

    def mate_copy(q):
        return pltpu.make_async_remote_copy(part.at[0], mate.at[q], ms.at[q], mr.at[q],
                                            device_id=mate_id, device_id_type=MESH)

    def chip_copy(q):
        return pltpu.make_async_remote_copy(ours.at[q], theirs.at[q], cs.at[q], cr.at[q],
                                            device_id={AXIS: 2 * owner_chip(q) + core}, device_id_type=MESH)

    gain = g_ref[...].astype(F32)

    def prep(c, carry):
        r = rows(c)
        load(c).wait()
        xf = x_v[r, :].astype(F32)
        inv = lax.rsqrt(jnp.mean(xf * xf, axis=-1, keepdims=True) + EPS)
        nb = (xf * inv * gain).astype(BF16)
        n_v[r, :] = nb
        nt_v[:, r] = nb.T
        y_v[r, :] = jnp.zeros((tc, d), F32)
        dn_v[r, :] = jnp.zeros((tc, d), F32)
        return carry

    hs, dus, dhs = (h_a, h_b), (du_a, du_b), (dh_a, dh_b)

    def pull(i, slot):
        j, c = block_of(lax.div(i, nc)), lax.rem(i, nc)
        return pltpu.make_async_copy(dh_hbm.at[j, rows(c)], dhs[slot], dh_sem.at[slot])

    for i in range(2):
        pull(i, i).start()
    lax.fori_loop(0, nc, prep, 0)
    for cp in weights:
        cp.wait()
    pl.semaphore_wait(pltpu.get_barrier_semaphore(), n - 1)

    steps = n * nc
    sub = tc // 4

    def first_piece(i, slot, k):
        j, c = block_of(lax.div(i, nc)), lax.rem(i, nc)
        here = pl.ds(k * sub, sub)
        u = dot_nn(n_v[pl.ds(pl.multiple_of(c * tc + k * sub, sub), sub), :], w1_ref[j]).astype(BF16).astype(F32)
        hs[slot][here, :], dus[slot][here, :] = gelu_pair(u, dhs[slot][here, :])

    def second_piece(i, slot, k):
        jj, c = lax.div(i, nc), lax.rem(i, nc)
        j, half = block_of(jj), lax.rem(jj, 2)
        r = rows(c)
        if k == 0:
            y_v[r, :] += dot_nn(hs[slot][...], w2_ref[j])
        elif k == 1:
            dn_v[r, :] += dot_nt(dus[slot][...], w1_ref[j])
        elif k == 2:
            part[half, 0] += dot_nn(nt_v[:, r], dus[slot][...])
        else:
            part[half, 1] += dot_nn(dot_v[:, r], hs[slot][...])

    def both(i, slot):
        pull(i + 1, 1 - slot).wait()
        for k in range(4):
            first_piece(i + 1, 1 - slot, k)
            second_piece(i, slot, k)

        @pl.when(i + 3 < steps)
        def _():
            pull(i + 3, 1 - slot).start()

    def opens(i):
        jj = lax.div(i, nc)
        q, half = lax.div(jj, 2), lax.rem(jj, 2)

        @pl.when(lax.rem(i, nc) == 0)
        def _():
            @pl.when((half == 0) & (q >= 1))
            def _():
                mate_copy(q - 1).wait_send()

            part[half] = jnp.zeros(part.shape[1:], F32)

    def closes(i):
        jj = lax.div(i, nc)
        q, half = lax.div(jj, 2), lax.rem(jj, 2)

        @pl.when((lax.rem(i, nc) == nc - 1) & (half == 0))
        def _():
            mate_copy(q).start()

        @pl.when((lax.rem(i, nc) == nc - 1) & (half == 1))
        def _():
            mate_copy(q).wait_recv()
            ours[q] = part[1] + mate[q]
            chip_copy(q).start()

    pull(0, 0).wait()
    for k in range(4):
        first_piece(0, 0, k)
    pull(2, 0).start()

    def body(m, carry):
        i = 2 * m
        opens(i)
        both(i, 0)
        both(i + 1, 1)
        closes(i + 1)
        return carry

    lax.fori_loop(0, steps // 2 - 1, body, 0)
    opens(steps - 2)
    both(steps - 2, 0)
    for k in range(4):
        second_piece(steps - 1, 1, k)
    mate_copy(chips - 1).wait_recv()
    late.wait()

    def tail(c, carry):
        r = rows(c)
        xf = x_v[r, :].astype(F32)
        inv = lax.rsqrt(jnp.mean(xf * xf, axis=-1, keepdims=True) + EPS)
        w = dn_v[r, :] * gain
        proj = jnp.mean(xf * w, axis=-1, keepdims=True) * (inv * inv * inv)
        dx = do_v[r, :].astype(F32) + (w * inv - xf * proj)
        do_v[r, :] = dx.astype(BF16)
        x_v[r, :] = (xf + y_v[r, :]).astype(BF16)
        pltpu.make_async_copy(do_v.at[r], dx_hbm.at[r], out_sem.at[1]).start()
        pltpu.make_async_copy(x_v.at[r], out_hbm.at[r], out_sem.at[0]).start()
        return carry

    lax.fori_loop(0, nc, tail, 0)
    total = part[1] + mate[chips - 1]
    for q in range(chips - 1):
        chip_copy(q).wait_recv()
        total = total + theirs[q]
    part[1] = total
    up = pltpu.make_async_copy(part.at[1, 0], dw1_hbm, dw_sem.at[0])
    down = pltpu.make_async_copy(part.at[1, 1], dw2_hbm, dw_sem.at[1])
    up.start()
    down.start()
    mate_copy(chips - 1).wait_send()
    for q in range(chips - 1):
        chip_copy(q).wait_send()
    up.wait()
    down.wait()
    pltpu.make_async_copy(do_v, dx_hbm, out_sem.at[1]).wait()
    pltpu.make_async_copy(x_v, out_hbm, out_sem.at[0]).wait()


def mlp(n, cid, x, g, w1s, w2s, dout, dh, dot, tc=1024):
    t, d = x.shape
    fs = w1s.shape[2]
    nc = t // tc
    chips = n // 2
    return pl.pallas_call(
        functools.partial(mlp_kernel, n, tc),
        out_shape=(
            jax.ShapeDtypeStruct((t, d), BF16),
            jax.ShapeDtypeStruct((t, d), BF16),
            jax.ShapeDtypeStruct((d, fs), F32),
            jax.ShapeDtypeStruct((d, fs), F32),
        ),
        in_specs=[any_spec(), vmem_spec()] + [any_spec()] * 5,
        out_specs=(any_spec(),) * 4,
        scratch_shapes=[
            pltpu.VMEM((t, d), BF16), pltpu.VMEM((t, d), BF16), pltpu.VMEM((t, d), BF16),
            pltpu.VMEM((d, t), BF16), pltpu.VMEM((d, t), BF16),
            pltpu.VMEM((t, d), F32), pltpu.VMEM((t, d), F32),
            pltpu.VMEM(w1s.shape, BF16), pltpu.VMEM(w2s.shape, BF16),
            pltpu.VMEM((tc, fs), BF16), pltpu.VMEM((tc, fs), BF16), pltpu.VMEM((tc, fs), BF16), pltpu.VMEM((tc, fs), BF16),
            pltpu.VMEM((tc, fs), F32), pltpu.VMEM((tc, fs), F32),
            pltpu.VMEM((2, 2, d, fs), F32), pltpu.VMEM((chips, 2, d, fs), F32),
            pltpu.VMEM((chips - 1, 2, d, fs), F32), pltpu.VMEM((chips - 1, 2, d, fs), F32),
            DMA((nc,)), DMA((4,)), DMA((2,)), DMA((2,)), DMA((2,)), DMA((chips,)), DMA((chips,)), DMA((chips,)), DMA((chips,)),
        ],
        compiler_params=pltpu.CompilerParams(
            collective_id=cid, has_side_effects=True, vmem_limit_bytes=63 << 20),
        cost_estimate=pl.CostEstimate(flops=12 * t * d * n * fs, bytes_accessed=40 << 20, transcendentals=t * n * fs),
        name='mlp_block',
    )(x, g.reshape(1, d), w1s, w2s, dout, dh, dot)


def share_kernel(n, pack, lists, ss, rs, own_sem):
    me = lax.axis_index(AXIS)
    pl_len = pack.shape[0]
    here = pl.ds(pl.multiple_of(me * pl_len, PAGE), pl_len)
    own = pltpu.make_async_copy(pack, lists.at[here], own_sem)
    own.start()
    group_barrier(n, me)

    def list_copy(k):
        return pltpu.make_async_remote_copy(pack, lists.at[here], ss.at[k], rs.at[k],
                                            device_id={AXIS: lax.rem(me + k, n)}, device_id_type=MESH)

    for k in far_first(n):
        list_copy(k).start()
    for k in far_first(n):
        list_copy(k).wait()
    own.wait()


def share(n, pack):
    return pl.pallas_call(
        functools.partial(share_kernel, n),
        out_shape=jax.ShapeDtypeStruct((n * pack.shape[0],), I32),
        in_specs=[any_spec()],
        out_specs=any_spec(),
        scratch_shapes=[DMA((n,)), DMA((n,)), DMA],
        compiler_params=pltpu.CompilerParams(collective_id=1, has_side_effects=True, vmem_limit_bytes=63 << 20),
        name='share_lists',
    )(pack)


def serve_kernel(n, c1, c2, rnd_ref, who_ref, lists, table, out, ls, e_st, ef, g, sent, l_sem, e_sem, o_sem):
    me, rnd = who_ref[0], rnd_ref[0]
    vocab, d = e_st.shape
    w = d // LANES
    asked = pltpu.make_async_copy(lists, ls, l_sem)
    asked.start()
    pl_len = ls.shape[0] // n
    head = pl_len - PAGE
    last = head - c1 - c2
    parts = e_sem.shape[0]
    step = vocab // parts

    def load(i):
        return pltpu.make_async_copy(table.at[pl.ds(i * step, step)], e_st.at[pl.ds(i * step, step)], e_sem.at[i])

    for i in range(parts):
        load(i).start()
    for i in range(parts):
        load(i).wait()
        split_rows(e_st.at[pl.ds(i * step, step)], ef, i * step, step)

    asked.wait()

    def source(q, carry):
        at1 = q * pl_len + jnp.minimum(ls[q * pl_len + head + me] + rnd * c1, last)
        at2 = q * pl_len + jnp.minimum(ls[q * pl_len + head + 16 + me] + rnd * c2, last)
        pick_rows(ef, g, 0, c1, w, lambda j: ls[at1 + j])
        pick_rows(ef, g, c1, c2, w, lambda j: ls[at2 + j])
        join_rows(g, sent.at[q], 0, c1 + c2)
        pltpu.make_async_copy(sent.at[q], out.at[q], o_sem).start()
        return carry

    lax.fori_loop(0, n, source, 0)
    pltpu.make_async_copy(sent, out, o_sem).wait()


def serve(n, c1, c2, rnd, who, lists, table):
    vocab, d = table.shape
    w = d // LANES
    c = c1 + c2
    parts = 3 if vocab % 48 == 0 else 1
    return pl.pallas_call(
        functools.partial(serve_kernel, n, c1, c2),
        out_shape=jax.ShapeDtypeStruct((n, c, d), BF16),
        in_specs=[smem_spec(), smem_spec(), any_spec(), any_spec()],
        out_specs=any_spec(),
        scratch_shapes=[pltpu.SMEM(lists.shape, I32), pltpu.VMEM((vocab, d), BF16), pltpu.VMEM((vocab * w, LANES), F32),
                        pltpu.VMEM((c * w, LANES), F32), pltpu.VMEM((n, c, d), BF16), DMA, DMA((parts,)), DMA],
        compiler_params=pltpu.CompilerParams(vmem_limit_bytes=63 << 20),
        name='serve_rows',
    )(rnd, who, lists, table)


def swap_kernel(n, arrays, *refs):
    srcs, dsts, (ss, rs) = refs[:arrays], refs[arrays:2 * arrays], refs[2 * arrays:]
    me = lax.axis_index(AXIS)
    group_barrier(n, me)

    def copy(a, k):
        p = lax.rem(me + k, n)
        return pltpu.make_async_remote_copy(srcs[a].at[p], dsts[a].at[me], ss.at[a, k], rs.at[a, k],
                                            device_id={AXIS: p}, device_id_type=MESH)

    for k in far_first(n):
        for a in range(arrays):
            copy(a, k).start()
    for k in far_first(n):
        for a in range(arrays):
            copy(a, k).wait()


def swap(n, cid, name, *arrays):
    m = len(arrays)
    return pl.pallas_call(
        functools.partial(swap_kernel, n, m),
        out_shape=tuple(jax.ShapeDtypeStruct(a.shape, a.dtype) for a in arrays),
        in_specs=[any_spec()] * m,
        out_specs=(any_spec(),) * m,
        scratch_shapes=[DMA((m, n)), DMA((m, n))],
        compiler_params=pltpu.CompilerParams(collective_id=cid, has_side_effects=True, vmem_limit_bytes=63 << 20),
        name=name,
    )(*arrays)


def swap_first_kernel(n, others, tc, sent, need, do_hbm, w2_hbm, got, most, dh_hbm, dot_hbm, do_v, w2_v, dot_v, dh_v,
                      peers, relay, ss, rs, ns, nr, xs_sem, xr_sem, in_sem, w_sem, dh_sem, dot_sem):
    me = lax.axis_index(AXIS)
    t, d = do_v.shape
    nc = t // tc
    rows = lambda c: pl.ds(pl.multiple_of(c * tc, tc), tc)
    hops = []
    for name, size in others:
        reach = 1
        while reach < size:
            hops.append((name, size, reach))
            reach *= 2

    def load(c):
        return pltpu.make_async_copy(do_hbm.at[rows(c)], do_v.at[rows(c)], in_sem.at[c])

    weights = pltpu.make_async_copy(w2_hbm, w2_v, w_sem)
    weights.start()
    for c in range(nc):
        load(c).start()
    sem = pltpu.get_barrier_semaphore()
    for k in range(1, n):
        pl.semaphore_signal(sem, inc=1, device_id={AXIS: lax.rem(me + k, n)}, device_id_type=MESH)
    for name, size, reach in hops:
        at = lax.axis_index(name)
        pl.semaphore_signal(sem, inc=1, device_id={name: lax.rem(at + size - reach, size)}, device_id_type=MESH)
    pl.semaphore_wait(sem, n - 1 + len(hops))

    def row_copy(k):
        p = lax.rem(me + k, n)
        return pltpu.make_async_remote_copy(sent.at[p], got.at[me], ss.at[k], rs.at[k],
                                            device_id={AXIS: p}, device_id_type=MESH)

    def need_copy(k):
        return pltpu.make_async_remote_copy(need, peers.at[k], ns.at[k], nr.at[k],
                                            device_id={AXIS: lax.rem(me + k, n)}, device_id_type=MESH)

    for k in far_first(n):
        need_copy(k).start()
    for k in far_first(n):
        row_copy(k).start()
    weights.wait()

    def put(i):
        return pltpu.make_async_copy(dh_v.at[lax.rem(i, 2)], dh_hbm.at[lax.rem(i, n), rows(lax.div(i, n))],
                                     dh_sem.at[lax.rem(i, 2)])

    def body(i, carry):
        c, j = lax.div(i, n), lax.rem(i, n)

        @pl.when(j == 0)
        def _():
            load(c).wait()
            dot_v[:, rows(c)] = do_v[rows(c), :].T

        @pl.when(i >= 2)
        def _():
            put(i - 2).wait()

        dh_v[lax.rem(i, 2)] = dot_nt(do_v[rows(c), :], w2_v[j])
        put(i).start()
        return carry

    steps = n * nc
    lax.fori_loop(0, steps, body, 0)
    turned = pltpu.make_async_copy(dot_v, dot_hbm, dot_sem)
    turned.start()
    top = need[...]
    for k in range(1, n):
        need_copy(k).wait_recv()
        top = jnp.maximum(top, peers[k])
    for i, (name, size, reach) in enumerate(hops):
        relay[2 * i] = top
        at = lax.axis_index(name)
        hop = pltpu.make_async_remote_copy(relay.at[2 * i], relay.at[2 * i + 1], xs_sem.at[i], xr_sem.at[i],
                                           device_id={name: lax.rem(at + reach, size)}, device_id_type=MESH)
        hop.start()
        hop.wait()
        top = jnp.maximum(top, relay[2 * i + 1])
    most[...] = top
    for i in range(steps - 2, steps):
        put(i).wait()
    turned.wait()
    for k in far_first(n):
        need_copy(k).wait_send()
        row_copy(k).wait()


def swap_first(n, others, sent, need, dout, w2s, tc=1024):
    t, d = dout.shape
    fs = w2s.shape[1]
    nc = t // tc
    hops = max(1, sum((size - 1).bit_length() for _, size in others))
    tile = (8, LANES)
    return pl.pallas_call(
        functools.partial(swap_first_kernel, n, others, tc),
        out_shape=(jax.ShapeDtypeStruct(sent.shape, sent.dtype), jax.ShapeDtypeStruct(tile, I32),
                   jax.ShapeDtypeStruct((n, t, fs), F32), jax.ShapeDtypeStruct((d, t), BF16)),
        in_specs=[any_spec(), vmem_spec(), any_spec(), any_spec()],
        out_specs=(any_spec(), vmem_spec(), any_spec(), any_spec()),
        scratch_shapes=[
            pltpu.VMEM((t, d), BF16), pltpu.VMEM(w2s.shape, BF16), pltpu.VMEM((d, t), BF16), pltpu.VMEM((2, tc, fs), F32),
            pltpu.VMEM((n,) + tile, I32), pltpu.VMEM((2 * hops,) + tile, I32),
            DMA((n,)), DMA((n,)), DMA((n,)), DMA((n,)), DMA((hops,)), DMA((hops,)), DMA((nc,)), DMA, DMA((2,)), DMA,
        ],
        compiler_params=pltpu.CompilerParams(collective_id=5, has_side_effects=True, vmem_limit_bytes=63 << 20),
        name='swap_first',
    )(sent, need, dout, w2s)


def expand_kernel(n, c, again, *refs):
    if again:
        who_ref, toks_h, lines_h, sent, got, x_prev, out, toks, lines, rb, rf, xg, x_out, i_sem, in_sem, o_sem, x_sem = refs
    else:
        who_ref, toks_h, lines_h, sent, got, out, toks, lines, rb, rf, xg, x_out, i_sem, in_sem, o_sem = refs
    me = who_ref[0]
    t, d = x_out.shape
    w = d // LANES
    idx = (pltpu.make_async_copy(toks_h, toks, i_sem.at[0]), pltpu.make_async_copy(lines_h, lines, i_sem.at[1]))
    for cp in idx:
        cp.start()
    own = pltpu.make_async_copy(sent.at[me], rb.at[me], in_sem.at[me])
    own.start()
    if again:
        prev = pltpu.make_async_copy(x_prev, x_out, x_sem)
        prev.start()

    def load(q):
        return pltpu.make_async_copy(got.at[q], rb.at[q], in_sem.at[q])

    for k in range(n):
        @pl.when(k != me)
        def _():
            load(k).start()
    if again:
        prev.wait()
        split_rows(x_out, xg, 0, t)

    def source(q, carry):
        load(q).wait()
        split_rows(rb.at[q], rf, q * c, c)
        return carry

    lax.fori_loop(0, n, source, 0)

    for cp in idx:
        cp.wait()

    def body(b, carry):
        vals = [rf[pl.ds(pl.multiple_of(lines[b * UNROLL + u], w), w), :] for u in range(UNROLL)]
        for u in range(UNROLL):
            xg[pl.ds(pl.multiple_of(toks[b * UNROLL + u], w), w), :] = vals[u]
        return carry

    lax.fori_loop(0, t // UNROLL, body, 0)
    step = t // 4
    for i in range(4):
        join_rows(xg.at[pl.ds(i * step * w, step * w)], x_out, i * step, step)
        part = pl.ds(i * step, step)
        pltpu.make_async_copy(x_out.at[part], out.at[part], o_sem).start()
    pltpu.make_async_copy(x_out, out, o_sem).wait()


def expand(n, rnd, who, toks, lines, sent, got, x_prev=None):
    again = x_prev is not None
    t = toks.shape[0]
    _, c, d = sent.shape
    w = d // LANES
    lines = lines - rnd[0] * (n * c * w)
    here = (lines >= 0) & (lines < n * c * w)
    toks, lines = jnp.where(here, toks, t * w), jnp.where(here, lines, 0)
    return pl.pallas_call(
        functools.partial(expand_kernel, n, c, again),
        out_shape=jax.ShapeDtypeStruct((t, d), BF16),
        in_specs=[smem_spec()] + [any_spec()] * (5 if again else 4),
        out_specs=any_spec(),
        scratch_shapes=[pltpu.SMEM((t,), I32), pltpu.SMEM((t,), I32),
                        pltpu.VMEM((n, c, d), BF16), pltpu.VMEM((n * c * w, LANES), F32),
                        pltpu.VMEM((t * w + 8, LANES), F32), pltpu.VMEM((t, d), BF16), DMA((2,)), DMA((n,)), DMA] + ([DMA] if again else []),
        compiler_params=pltpu.CompilerParams(vmem_limit_bytes=63 << 20),
        name='expand_more' if again else 'expand_rows',
    )(who, toks, lines, sent, got, *((x_prev,) if again else ()))


def collect_kernel(n, c1, c2, vocab, again, *refs):
    if again:
        rnd_ref, pack_h, toks_h, ids, dx_hbm, one_out, many_out, *rest = refs
    else:
        rnd_ref, pack_h, toks_h, ids, dx_hbm, y_in, up_in, down_in, one_out, many_out, y_out, up_out, down_out, *rest = refs
        *rest, y_v, up_v, down_v, side_v, side_sem = rest
    pack, toks, dx_v, dxf, g, col, one, many, i_sem, in_sem, o_sem = rest
    rnd = rnd_ref[0]
    t, d = dx_v.shape
    w = d // LANES
    parts = in_sem.shape[0]
    step = t // parts
    head = pack.shape[0] - PAGE
    last = head - c1 - c2

    def load(i):
        rows = pl.ds(pl.multiple_of(i * step, step), step)
        return pltpu.make_async_copy(dx_hbm.at[rows], dx_v.at[rows], in_sem.at[i])

    idx = (pltpu.make_async_copy(pack_h, pack, i_sem.at[0]), pltpu.make_async_copy(toks_h, toks, i_sem.at[1]))
    for cp in idx:
        cp.start()
    for i in range(parts):
        load(i).start()
    if not again:
        side_in = (pltpu.make_async_copy(y_in, y_v, side_sem.at[0]), pltpu.make_async_copy(up_in, up_v, side_sem.at[1]),
                   pltpu.make_async_copy(down_in, down_v, side_sem.at[2]))
        side_out = (pltpu.make_async_copy(y_v, y_out, side_sem.at[0]), pltpu.make_async_copy(up_v, up_out, side_sem.at[1]),
                    pltpu.make_async_copy(side_v, down_out, side_sem.at[2]))
        for cp in side_in:
            cp.start()
    for cp in idx:
        cp.wait()

    def name_rows(q, carry):
        at = jnp.minimum(pack[head + 16 + q] + rnd * c2, last)
        for j in range(c2):
            col[pl.ds(q * c2 + j, 1), :] = jnp.full((1, LANES), pack[at + j] + q * (vocab * w), I32)
        return carry

    lax.fori_loop(0, n, name_rows, 0)
    many[...] = jnp.zeros(many.shape, F32)
    names = col[:, :1]

    def sum_many(i, carry):
        load(i).wait()
        hot = jnp.where(names == ids[i] * w, 1.0, 0.0).astype(BF16)
        rows = pl.ds(pl.multiple_of(i * step, step), step)
        many[...] += lax.dot_general(hot, dx_v[rows, :], (((1,), (0,)), ((), ())), preferred_element_type=F32)
        split_rows(dx_v.at[rows], dxf, i * step, step)
        return carry

    lax.fori_loop(0, parts, sum_many, 0)
    pltpu.make_async_copy(many, many_out, o_sem.at[1]).start()
    if not again:
        for cp in side_in:
            cp.wait()
        side_v[...] = down_v[...].T
        for cp in side_out:
            cp.start()

    def owner(q, carry):
        at = jnp.minimum(pack[head + q] + rnd * c1, last)
        pick_rows(dxf, g, 0, c1, w, lambda j: toks[at + j])
        join_rows(g, one.at[q], 0, c1)
        pltpu.make_async_copy(one.at[q], one_out.at[q], o_sem.at[0]).start()
        return carry

    lax.fori_loop(0, n, owner, 0)
    pltpu.make_async_copy(one, one_out, o_sem.at[0]).wait()
    pltpu.make_async_copy(many, many_out, o_sem.at[1]).wait()
    if not again:
        for cp in side_out:
            cp.wait()


def collect(n, c1, c2, vocab, rnd, pack, toks, ids, dx, side=None):
    again = side is None
    t, d = dx.shape
    w = d // LANES
    parts = ids.shape[0]
    shapes = (jax.ShapeDtypeStruct((n, c1, d), BF16), jax.ShapeDtypeStruct((n * c2, d), F32))
    extra = []
    if not again:
        y, up, down = side
        shapes += (jax.ShapeDtypeStruct(y.shape, y.dtype), jax.ShapeDtypeStruct(up.shape, F32),
                   jax.ShapeDtypeStruct(down.shape[::-1], F32))
        extra = [pltpu.VMEM(y.shape, y.dtype), pltpu.VMEM(up.shape, F32), pltpu.VMEM(down.shape, F32),
                 pltpu.VMEM(down.shape[::-1], F32), DMA((3,))]
    one, many, *rest = pl.pallas_call(
        functools.partial(collect_kernel, n, c1, c2, vocab, again),
        out_shape=shapes,
        in_specs=[smem_spec(), any_spec(), any_spec(), vmem_spec(), any_spec()] + [any_spec()] * (0 if again else 3),
        out_specs=(any_spec(),) * len(shapes),
        scratch_shapes=[pltpu.SMEM(pack.shape, I32), pltpu.SMEM(toks.shape, I32),
                        pltpu.VMEM((t, d), BF16), pltpu.VMEM((t * w, LANES), F32), pltpu.VMEM((c1 * w, LANES), F32),
                        pltpu.VMEM((n * c2, LANES), I32), pltpu.VMEM((n, c1, d), BF16), pltpu.VMEM((n * c2, d), F32),
                        DMA((2,)), DMA((parts,)), DMA((2,))] + extra,
        compiler_params=pltpu.CompilerParams(vmem_limit_bytes=63 << 20),
        name='collect_more' if again else 'collect_rows',
    )(rnd, pack, toks, ids, dx, *(() if again else side))
    return (one, many.reshape(n, c2, d)) + tuple(rest)


def place_kernel(n, c1, c2, again, *refs):
    if again:
        rnd_ref, who_ref, lists, one_own, many_own, one, many, _, out, ls, acc, o_v, m_v, f_v, st, l_sem, in_sem, out_sem = refs
    else:
        rnd_ref, who_ref, lists, one_own, many_own, one, many, out, ls, acc, o_v, m_v, f_v, st, l_sem, in_sem, out_sem = refs
    me, rnd = who_ref[0], rnd_ref[0]
    vocab, d = out.shape
    w = d // LANES
    asked = pltpu.make_async_copy(lists, ls, l_sem)
    asked.start()
    pl_len = ls.shape[0] // n
    head = pl_len - PAGE

    def load(q):
        return (pltpu.make_async_copy(one.at[q], o_v.at[q], in_sem.at[0, q]),
                pltpu.make_async_copy(many.at[q], m_v.at[q], in_sem.at[1, q]))

    pltpu.make_async_copy(one_own.at[me], o_v.at[me], in_sem.at[0, me]).start()
    pltpu.make_async_copy(many_own.at[me], m_v.at[me], in_sem.at[1, me]).start()
    for k in range(n):
        @pl.when(k != me)
        def _():
            for part in load(k):
                part.start()
    blk = st.shape[1]

    def span(i):
        return pl.ds(pl.multiple_of(i * blk, blk), blk)

    def split8(src, row):
        def one8(r0):
            for k in range(w):
                acc[pl.ds((row + r0) * w + k, 8, stride=w), :] = src[pl.ds(r0, 8), pl.ds(k * LANES, LANES)]
        blocks(blk, 8, 8, one8)

    if again:
        def bring(i, carry):
            pltpu.make_async_copy(out.at[span(i)], st.at[0], out_sem.at[0]).start()
            pltpu.make_async_copy(out.at[span(i)], st.at[0], out_sem.at[0]).wait()
            split8(st.at[0], i * blk)
            return carry

        lax.fori_loop(0, vocab // blk, bring, 0)
    else:
        zero = jnp.zeros((16 * w, LANES), F32)

        def clear(r0):
            acc[pl.ds(r0 * w, 16 * w), :] = zero

        blocks(vocab, 16, 4, clear)
    asked.wait()
    dump = vocab * w

    def add(count, at, row0):
        def body(b, carry):
            lines, sums = [], []
            for u in range(UNROLL):
                j = b * UNROLL + u
                line = pl.multiple_of(jnp.where(j < count, ls[at + j], dump), w)
                lines.append(line)
                src = f_v[pl.ds(pl.multiple_of((row0 + j) * w, w), w), :]
                sums.append(acc[pl.ds(line, w), :] + src)
            for u in range(UNROLL):
                acc[pl.ds(lines[u], w), :] = sums[u]
            return carry

        lax.fori_loop(0, lax.div(count + UNROLL - 1, UNROLL), body, 0)

    def source(q, carry):
        for part in load(q):
            part.wait()
        at = q * pl_len + head
        split_rows(o_v.at[q], f_v, 0, c1)
        split_rows(m_v.at[q], f_v, c1, c2)
        b1, b2 = ls[at + me] + rnd * c1, ls[at + 16 + me] + rnd * c2
        e1, e2 = ls[at + me + 1], ls[at + 16 + me + 1]
        add(jnp.clip(e1 - b1, 0, c1), q * pl_len + b1, 0)
        add(jnp.clip(e2 - b2, 0, c2), q * pl_len + b2, c1)
        return carry

    lax.fori_loop(0, n, source, 0)

    def emit(i, carry):
        slot = lax.rem(i, 2)

        @pl.when(i >= 2)
        def _():
            pltpu.make_async_copy(st.at[slot], out.at[span(i - 2)], out_sem.at[slot]).wait()

        def one8(r0):
            for k in range(w):
                st[slot, pl.ds(r0, 8), pl.ds(k * LANES, LANES)] = acc[pl.ds((i * blk + r0) * w + k, 8, stride=w), :]

        blocks(blk, 8, 8, one8)
        pltpu.make_async_copy(st.at[slot], out.at[span(i)], out_sem.at[slot]).start()
        return carry

    total = vocab // blk
    lax.fori_loop(0, total, emit, 0)
    for i in range(max(0, total - 2), total):
        pltpu.make_async_copy(st.at[i % 2], out.at[span(i)], out_sem.at[i % 2]).wait()


def place(n, c1, c2, vocab, rnd, who, lists, one_own, many_own, one, many, prev=None):
    again = prev is not None
    d = one.shape[-1]
    w = d // LANES
    blk = next(b for b in range(1280, 0, -8) if vocab % b == 0)
    return pl.pallas_call(
        functools.partial(place_kernel, n, c1, c2, again),
        out_shape=jax.ShapeDtypeStruct((vocab, d), F32),
        in_specs=[smem_spec()] * 2 + [any_spec()] * (6 if again else 5),
        out_specs=any_spec(),
        scratch_shapes=[
            pltpu.SMEM(lists.shape, I32), pltpu.VMEM((vocab * w + 8, LANES), F32), pltpu.VMEM((n, c1, d), BF16), pltpu.VMEM((n, c2, d), F32),
            pltpu.VMEM(((c1 + c2) * w, LANES), F32), pltpu.VMEM((2, blk, d), F32), DMA, DMA((2, n)), DMA((2,)),
        ],
        input_output_aliases={7: 0} if again else {},
        compiler_params=pltpu.CompilerParams(vmem_limit_bytes=63 << 20),
        name='place_more' if again else 'place_rows',
    )(rnd, who, lists, one_own, many_own, one, many, *((prev,) if again else ()))


def route(n, vocab, w, c1, c2, ids):
    t = ids.shape[0]
    c = c1 + c2
    s, p = lax.sort((ids, lax.iota(I32, t)), num_keys=1)
    edge = jnp.full((1,), -1, I32)
    first = s != jnp.concatenate([edge, s[:-1]])
    last = s != jnp.concatenate([s[1:], edge])
    lone = first & last
    lead = first & ~last
    lone_i, lead_i = lone.astype(I32), lead.astype(I32)
    bounds = lax.iota(I32, n + 1) * vocab
    below = s[None, :] < bounds[:, None]
    base1 = jnp.sum(jnp.where(below, lone_i[None, :], 0), axis=1)
    base2 = jnp.sum(jnp.where(below, lead_i[None, :], 0), axis=1)
    owner = n - jnp.sum(below[1:].astype(I32), axis=0)
    mine = owner[None, :] == lax.iota(I32, n)[:, None]
    start1 = jnp.sum(jnp.where(mine, base1[:n, None], 0), axis=0)
    start2 = jnp.sum(jnp.where(mine, base2[:n, None], 0), axis=0)
    r1 = jnp.cumsum(lone_i) - lone_i - start1
    r2 = jnp.cumsum(lead_i) - 1 - start2
    rnd1, rnd2 = r1 // c1, r2 // c2
    slot = jnp.where(lone, rnd1 * (n * c) + owner * c + r1 - rnd1 * c1, rnd2 * (n * c) + owner * c + c1 + r2 - rnd2 * c2)
    kind = jnp.where(lone, 0, jnp.where(lead, 1, 2)) * t + lax.iota(I32, t)
    _, line, tok = lax.sort((kind, (s - owner * vocab) * w, p * w), num_keys=1)
    n1 = base1[n]
    room = -(-(t + c1 + c2) // PAGE) * PAGE
    spare = jnp.zeros((16 - n - 1,), I32)
    heads = jnp.concatenate([base1, spare, n1 + base2, spare])
    fill = jnp.zeros((room - t,), I32)
    heads = jnp.concatenate([heads, jnp.zeros((PAGE - heads.shape[0],), I32)])
    pack = jnp.concatenate([line, fill, heads])
    lone_tok = jnp.concatenate([tok, fill])
    per1 = jnp.max(base1[1:] - base1[:-1])
    per2 = jnp.max(base2[1:] - base2[:-1])
    rounds = jnp.maximum((per1 + c1 - 1) // c1, (per2 + c2 - 1) // c2)
    return pack, lone_tok, p * w, slot * w, rounds


def solution(mesh):
    n = mesh.shape[AXIS]
    axes = tuple(mesh.axis_names)
    others = tuple((name, mesh.shape[name]) for name in axes if name != AXIS)
    tok_spec = P(axes)
    row_spec = P(axes, None)

    def local_step(token_ids, emb_shard, norm_gain, w_up_l, w_down_l, grad_out):
        vocab, d = emb_shard.shape
        t = token_ids.shape[0]
        w = d // LANES
        c1 = -(-(t * 5 // (8 * n)) // 16) * 16
        c2 = -(-(t // 128) // 16) * 16
        who = lax.axis_index(AXIS)[None].astype(I32)
        w_up = lax.all_gather(w_up_l, AXIS)
        w_down = lax.all_gather(w_down_l, AXIS)
        pack, lone_tok, toks, lines, rounds = route(n, vocab, w, c1, c2, token_ids)
        lists = share(n, pack)
        none = jnp.zeros((1,), I32)

        def rows_of(rnd):
            sent = serve(n, c1, c2, rnd, who, lists, emb_shard)
            return sent, swap(n, 2, 'swap_rows', sent)[0]

        def more_rows(carry):
            r, x_now = carry
            return r + 1, expand(n, r[None], who, toks, lines, *rows_of(r[None]), x_now)

        sent = serve(n, c1, c2, none, who, lists, emb_shard)
        got, most, dh, dot = swap_first(n, others, sent, jnp.full((8, LANES), rounds, I32), grad_out, w_down)
        rounds = most[0, 0]
        x = expand(n, none, who, toks, lines, sent, got)
        _, x = lax.while_loop(lambda carry: carry[0] < rounds, more_rows, (jnp.ones((), I32), x))
        out, dx, dw1, dw2t = mlp(n, 4, x, norm_gain, w_up, w_down, grad_out, dh, dot)
        ids_c = token_ids.reshape(-1, 1, t // 8)

        one, many, out, dw1, dw2 = collect(n, c1, c2, vocab, none, pack, lone_tok, ids_c, dx, (out, dw1, dw2t))

        def more_sums(carry):
            r, now = carry
            mine = collect(n, c1, c2, vocab, r[None], pack, lone_tok, ids_c, dx)
            return r + 1, place(n, c1, c2, vocab, r[None], who, lists, *mine, *swap(n, 3, 'swap_sums', *mine), now)

        d_emb = place(n, c1, c2, vocab, none, who, lists, one, many, *swap(n, 3, 'swap_sums', one, many))
        _, d_emb = lax.while_loop(lambda carry: carry[0] < rounds, more_sums, (jnp.ones((), I32), d_emb))
        return out, d_emb, dw1, dw2

    return jax.shard_map(
        local_step,
        mesh=mesh,
        in_specs=(tok_spec, P(AXIS, None), P(None), P(None, AXIS), P(AXIS, None), row_spec),
        out_specs=(row_spec, row_spec, P(axes[0], AXIS), row_spec),
        check_vma=False,
    )
```

```python
import functools

import jax
import jax.numpy as jnp
from jax import lax
from jax.experimental import pallas as pl
from jax.experimental.pallas import tpu as pltpu
from jax.sharding import PartitionSpec as P

EPS = 1e-6
F32 = jnp.float32
BF16 = jnp.bfloat16
I32 = jnp.int32
MESH = pl.DeviceIdType.MESH
LANES = 128
UNROLL = 32
UNROLL_ADD = 8
PAGE = 1024
AXIS = 'tensor'


def group_barrier(n, me, wait=True):
    sem = pltpu.get_barrier_semaphore()
    for k in range(1, n):
        pl.semaphore_signal(sem, inc=1, device_id={AXIS: lax.rem(me + k, n)}, device_id_type=MESH)
    if wait:
        pl.semaphore_wait(sem, n - 1)


def far_first(n):
    return sorted(range(1, n), key=lambda k: -min(k // 2, (n - k) // 2))


def blocks(count, size, many, one):
    total = count // size

    def body(b, carry):
        for u in range(many):
            one(pl.multiple_of((b * many + u) * size, size))
        return carry

    lax.fori_loop(0, total // many, body, 0)
    for b in range(total // many * many, total):
        one(b * size)


def split_rows(src, dst, dst_row, count):
    w = src.shape[-1] // LANES

    def one(r0):
        tile = src[pl.ds(r0, 16), :].astype(F32)
        for c in range(w):
            dst[pl.ds((dst_row + r0) * w + c, 16, stride=w), :] = tile[:, c * LANES:(c + 1) * LANES]

    blocks(count, 16, 4, one)


def join_rows(src, dst, dst_row, count):
    w = dst.shape[-1] // LANES

    def one(r0):
        parts = [src[pl.ds(r0 * w + c, 16, stride=w), :] for c in range(w)]
        dst[pl.ds(pl.multiple_of(dst_row + r0, 16), 16), :] = jnp.concatenate(parts, axis=1).astype(dst.dtype)

    blocks(count, 16, 4, one)


def pick_rows(src, dst, dst_row, count, w, index):
    def body(b, carry):
        vals = []
        for u in range(UNROLL):
            line = pl.multiple_of(index(b * UNROLL + u), w)
            vals.append(src[pl.ds(line, w), :])
        for u in range(UNROLL):
            dst[pl.ds(pl.multiple_of((dst_row + b * UNROLL + u) * w, w), w), :] = vals[u]
        return carry

    lax.fori_loop(0, count // UNROLL, body, 0)


def any_spec():
    return pl.BlockSpec(memory_space=pltpu.HBM)


def smem_spec():
    return pl.BlockSpec(memory_space=pltpu.SMEM)


def vmem_spec():
    return pl.BlockSpec(memory_space=pltpu.VMEM)


DMA = pltpu.SemaphoreType.DMA


K0 = 0.7978845608028654
K1 = 0.044715


def dot_nn(a, b):
    return lax.dot_general(a, b, (((1,), (0,)), ((), ())), preferred_element_type=F32)


def dot_nt(a, b):
    return lax.dot_general(a, b, (((1,), (1,)), ((), ())), preferred_element_type=F32)


def gelu_pair(u, dh):
    u2 = u * u
    t = jnp.tanh(u * (K0 + (K0 * K1) * u2))
    s = 0.5 + 0.5 * t
    h = u * s
    slope = s + h * (1.0 - s) * (2.0 * K0 + (6.0 * K0 * K1) * u2)
    return h.astype(BF16), (dh * slope).astype(BF16)


def mlp_kernel(n, tc, x_hbm, g_ref, w_hbm, do_hbm, dh_hbm, dot_hbm, out_hbm, dx_hbm, dw1_hbm, dw2_hbm,
               x_v, do_v, n_v, nt_v, dot_v, y_v, dn_v, w_ref, h_a, h_b, du_a, du_b, dh_a, dh_b, part, mate, ours, theirs,
               in_sem, w_sem, dh_sem, out_sem, dw_sem, ms, mr, cs, cr):
    me = lax.axis_index(AXIS)
    core, chip = lax.rem(me, 2), lax.div(me, 2)
    chips = n // 2
    far = sorted(range(1, chips), key=lambda k: -min(k, chips - k)) + [0]
    t_all, d = x_v.shape
    fs = w_ref.shape[2] // 2
    nc = t_all // tc
    rows = lambda c: pl.ds(pl.multiple_of(c * tc, tc), tc)
    mate_id = {AXIS: me + 1 - 2 * core}

    def load(c):
        r = rows(c)
        return pltpu.make_async_copy(x_hbm.at[r], x_v.at[r], in_sem.at[c])

    for c in range(nc):
        load(c).start()
    weights = (pltpu.make_async_copy(w_hbm, w_ref, w_sem.at[0]), pltpu.make_async_copy(dot_hbm, dot_v, w_sem.at[2]))
    for cp in weights:
        cp.start()
    group_barrier(n, me, wait=False)
    late = pltpu.make_async_copy(do_hbm, do_v, w_sem.at[3])
    late.start()

    def offset(q, which):
        off = sum(jnp.where(q == i, k, 0) for i, k in enumerate(far))
        return jnp.where(which == 0, off, lax.rem(chips - off, chips))

    def owner_chip(q):
        return lax.rem(chip + offset(q, core), chips)

    def block_of(jj):
        half = lax.rem(jj, 2)
        return 1 - half, offset(lax.div(jj, 2), jnp.where(half == 0, 1 - core, core))

    def mate_copy(q):
        return pltpu.make_async_remote_copy(part.at[0], mate.at[q], ms.at[q], mr.at[q],
                                            device_id=mate_id, device_id_type=MESH)

    def chip_copy(q):
        return pltpu.make_async_remote_copy(ours.at[q], theirs.at[q], cs.at[q], cr.at[q],
                                            device_id={AXIS: 2 * owner_chip(q) + core}, device_id_type=MESH)

    gain = g_ref[...].astype(F32)

    def prep(c, carry):
        r = rows(c)
        load(c).wait()
        xf = x_v[r, :].astype(F32)
        inv = lax.rsqrt(jnp.mean(xf * xf, axis=-1, keepdims=True) + EPS)
        nb = (xf * inv * gain).astype(BF16)
        n_v[r, :] = nb
        nt_v[:, r] = nb.T
        y_v[r, :] = jnp.zeros((tc, d), F32)
        dn_v[r, :] = jnp.zeros((tc, d), F32)
        return carry

    hs, dus, dhs = (h_a, h_b), (du_a, du_b), (dh_a, dh_b)

    def pull(i, slot):
        (side, rel), c = block_of(lax.div(i, nc)), lax.rem(i, nc)
        return pltpu.make_async_copy(dh_hbm.at[side * chips + rel, rows(c)], dhs[slot], dh_sem.at[slot])

    for i in range(2):
        pull(i, i).start()
    lax.fori_loop(0, nc, prep, 0)
    for cp in weights:
        cp.wait()
    pl.semaphore_wait(pltpu.get_barrier_semaphore(), n - 1)

    steps = n * nc
    sub = tc // 4

    def first_piece(i, slot, k):
        (side, rel), c = block_of(lax.div(i, nc)), lax.rem(i, nc)
        here = pl.ds(k * sub, sub)
        u = dot_nt(n_v[pl.ds(pl.multiple_of(c * tc + k * sub, sub), sub), :], w_ref[side, rel, pl.ds(0, fs), :])
        u = u.astype(BF16).astype(F32)
        hs[slot][here, :], dus[slot][here, :] = gelu_pair(u, dhs[slot][here, :])

    def second_piece(i, slot, k):
        jj, c = lax.div(i, nc), lax.rem(i, nc)
        (side, rel), half = block_of(jj), lax.rem(jj, 2)
        r = rows(c)
        if k == 0:
            y_v[r, :] += dot_nn(hs[slot][...], w_ref[side, rel, pl.ds(fs, fs), :])
        elif k == 1:
            dn_v[r, :] += dot_nn(dus[slot][...], w_ref[side, rel, pl.ds(0, fs), :])
        elif k == 2:
            part[half, 0] += dot_nn(nt_v[:, r], dus[slot][...])
        else:
            part[half, 1] += dot_nn(dot_v[:, r], hs[slot][...])

    def both(i, slot):
        pull(i + 1, 1 - slot).wait()
        for k in range(4):
            first_piece(i + 1, 1 - slot, k)
            second_piece(i, slot, k)

        @pl.when(i + 3 < steps)
        def _():
            pull(i + 3, 1 - slot).start()

    def opens(i):
        jj = lax.div(i, nc)
        q, half = lax.div(jj, 2), lax.rem(jj, 2)

        @pl.when(lax.rem(i, nc) == 0)
        def _():
            @pl.when((half == 0) & (q >= 1))
            def _():
                mate_copy(q - 1).wait_send()

            part[half] = jnp.zeros(part.shape[1:], F32)

    def closes(i):
        jj = lax.div(i, nc)
        q, half = lax.div(jj, 2), lax.rem(jj, 2)

        @pl.when((lax.rem(i, nc) == nc - 1) & (half == 0))
        def _():
            mate_copy(q).start()

        @pl.when((lax.rem(i, nc) == nc - 1) & (half == 1))
        def _():
            mate_copy(q).wait_recv()
            ours[q] = part[1] + mate[q]
            chip_copy(q).start()

    pull(0, 0).wait()
    for k in range(4):
        first_piece(0, 0, k)
    pull(2, 0).start()

    def body(m, carry):
        i = 2 * m
        opens(i)
        both(i, 0)
        both(i + 1, 1)
        closes(i + 1)
        return carry

    lax.fori_loop(0, steps // 2 - 1, body, 0)
    opens(steps - 2)
    both(steps - 2, 0)
    for k in range(4):
        second_piece(steps - 1, 1, k)
    mate_copy(chips - 1).wait_recv()
    late.wait()

    def tail(c, carry):
        r = rows(c)
        xf = x_v[r, :].astype(F32)
        inv = lax.rsqrt(jnp.mean(xf * xf, axis=-1, keepdims=True) + EPS)
        w = dn_v[r, :] * gain
        proj = jnp.mean(xf * w, axis=-1, keepdims=True) * (inv * inv * inv)
        dx = do_v[r, :].astype(F32) + (w * inv - xf * proj)
        do_v[r, :] = dx.astype(BF16)
        x_v[r, :] = (xf + y_v[r, :]).astype(BF16)
        pltpu.make_async_copy(do_v.at[r], dx_hbm.at[r], out_sem.at[1]).start()
        pltpu.make_async_copy(x_v.at[r], out_hbm.at[r], out_sem.at[0]).start()
        return carry

    lax.fori_loop(0, nc, tail, 0)
    total = part[1] + mate[chips - 1]
    for q in range(chips - 1):
        chip_copy(q).wait_recv()
        total = total + theirs[q]
    part[1] = total
    up = pltpu.make_async_copy(part.at[1, 0], dw1_hbm, dw_sem.at[0])
    down = pltpu.make_async_copy(part.at[1, 1], dw2_hbm, dw_sem.at[1])
    up.start()
    down.start()
    mate_copy(chips - 1).wait_send()
    for q in range(chips - 1):
        chip_copy(q).wait_send()
    up.wait()
    down.wait()
    pltpu.make_async_copy(do_v, dx_hbm, out_sem.at[1]).wait()
    pltpu.make_async_copy(x_v, out_hbm, out_sem.at[0]).wait()


def mlp(n, cid, x, g, ws, dout, dh, dot, tc=1024):
    t, d = x.shape
    fs = dh.shape[2]
    nc = t // tc
    chips = n // 2
    return pl.pallas_call(
        functools.partial(mlp_kernel, n, tc),
        out_shape=(
            jax.ShapeDtypeStruct((t, d), BF16),
            jax.ShapeDtypeStruct((t, d), BF16),
            jax.ShapeDtypeStruct((d, fs), F32),
            jax.ShapeDtypeStruct((d, fs), F32),
        ),
        in_specs=[any_spec(), vmem_spec()] + [any_spec()] * 4,
        out_specs=(any_spec(),) * 4,
        scratch_shapes=[
            pltpu.VMEM((t, d), BF16), pltpu.VMEM((t, d), BF16), pltpu.VMEM((t, d), BF16),
            pltpu.VMEM((d, t), BF16), pltpu.VMEM((d, t), BF16),
            pltpu.VMEM((t, d), F32), pltpu.VMEM((t, d), F32),
            pltpu.VMEM(ws.shape, BF16),
            pltpu.VMEM((tc, fs), BF16), pltpu.VMEM((tc, fs), BF16), pltpu.VMEM((tc, fs), BF16), pltpu.VMEM((tc, fs), BF16),
            pltpu.VMEM((tc, fs), F32), pltpu.VMEM((tc, fs), F32),
            pltpu.VMEM((2, 2, d, fs), F32), pltpu.VMEM((chips, 2, d, fs), F32),
            pltpu.VMEM((chips - 1, 2, d, fs), F32), pltpu.VMEM((chips - 1, 2, d, fs), F32),
            DMA((nc,)), DMA((4,)), DMA((2,)), DMA((2,)), DMA((2,)), DMA((chips,)), DMA((chips,)), DMA((chips,)), DMA((chips,)),
        ],
        compiler_params=pltpu.CompilerParams(
            collective_id=cid, has_side_effects=True, vmem_limit_bytes=63 << 20),
        cost_estimate=pl.CostEstimate(flops=12 * t * d * n * fs, bytes_accessed=40 << 20, transcendentals=t * n * fs),
        name='mlp_block',
    )(x, g.reshape(1, d), ws, dout, dh, dot)


def share_kernel(n, fs, pack, behind, before, lists, across, ss, rs, own_sem, fs_sem, fr_sem):
    me = lax.axis_index(AXIS)
    pl_len = pack.shape[0]
    here = pl.ds(pl.multiple_of(me * pl_len, PAGE), pl_len)
    own = pltpu.make_async_copy(pack, lists.at[here], own_sem)
    own.start()
    group_barrier(n, me)

    def list_copy(k):
        return pltpu.make_async_remote_copy(pack, lists.at[here], ss.at[k], rs.at[k],
                                            device_id={AXIS: lax.rem(me + k, n)}, device_id_type=MESH)

    def forward(way, src):
        half = pl.ds(way * fs, fs)
        return pltpu.make_async_remote_copy(src.at[half], across.at[half], fs_sem.at[way], fr_sem.at[way],
                                            device_id={AXIS: lax.rem(me + (2 if way == 0 else n - 2), n)}, device_id_type=MESH)

    for k in far_first(n):
        list_copy(k).start()
    forward(0, behind).start()
    forward(1, before).start()
    for k in far_first(n):
        list_copy(k).wait()
    own.wait()
    forward(0, behind).wait()
    forward(1, before).wait()


def share(n, pack, behind, before):
    return pl.pallas_call(
        functools.partial(share_kernel, n, behind.shape[0] // 2),
        out_shape=(jax.ShapeDtypeStruct((n * pack.shape[0],), I32), jax.ShapeDtypeStruct(behind.shape, BF16)),
        in_specs=[any_spec()] * 3,
        out_specs=(any_spec(),) * 2,
        scratch_shapes=[DMA((n,)), DMA((n,)), DMA, DMA((2,)), DMA((2,))],
        compiler_params=pltpu.CompilerParams(collective_id=1, has_side_effects=True, vmem_limit_bytes=63 << 20),
        name='share_lists',
    )(pack, behind, before)


def serve_kernel(n, c1, c2, rnd_ref, who_ref, lists, table, out, ls, e_st, ef, g, sent, l_sem, e_sem, o_sem):
    me, rnd = who_ref[0], rnd_ref[0]
    vocab, d = e_st.shape
    w = d // LANES
    asked = pltpu.make_async_copy(lists, ls, l_sem)
    asked.start()
    pl_len = ls.shape[0] // n
    head = pl_len - PAGE
    last = head - c1 - c2
    parts = e_sem.shape[0]
    step = vocab // parts

    def load(i):
        return pltpu.make_async_copy(table.at[pl.ds(i * step, step)], e_st.at[pl.ds(i * step, step)], e_sem.at[i])

    for i in range(parts):
        load(i).start()
    for i in range(parts):
        load(i).wait()
        split_rows(e_st.at[pl.ds(i * step, step)], ef, i * step, step)

    asked.wait()

    def source(q, carry):
        at1 = q * pl_len + jnp.minimum(ls[q * pl_len + head + me] + rnd * c1, last)
        at2 = q * pl_len + jnp.minimum(ls[q * pl_len + head + 16 + me] + rnd * c2, last)
        pick_rows(ef, g, 0, c1, w, lambda j: ls[at1 + j])
        pick_rows(ef, g, c1, c2, w, lambda j: ls[at2 + j])
        join_rows(g, sent.at[q], 0, c1 + c2)
        pltpu.make_async_copy(sent.at[q], out.at[q], o_sem).start()
        return carry

    lax.fori_loop(0, n, source, 0)
    pltpu.make_async_copy(sent, out, o_sem).wait()


def serve(n, c1, c2, rnd, who, lists, table):
    vocab, d = table.shape
    w = d // LANES
    c = c1 + c2
    parts = 3 if vocab % 48 == 0 else 1
    return pl.pallas_call(
        functools.partial(serve_kernel, n, c1, c2),
        out_shape=jax.ShapeDtypeStruct((n, c, d), BF16),
        in_specs=[smem_spec(), smem_spec(), any_spec(), any_spec()],
        out_specs=any_spec(),
        scratch_shapes=[pltpu.SMEM(lists.shape, I32), pltpu.VMEM((vocab, d), BF16), pltpu.VMEM((vocab * w, LANES), F32),
                        pltpu.VMEM((c * w, LANES), F32), pltpu.VMEM((n, c, d), BF16), DMA, DMA((parts,)), DMA],
        compiler_params=pltpu.CompilerParams(vmem_limit_bytes=63 << 20),
        name='serve_rows',
    )(rnd, who, lists, table)


def swap_kernel(n, arrays, *refs):
    srcs, dsts, (ss, rs) = refs[:arrays], refs[arrays:2 * arrays], refs[2 * arrays:]
    me = lax.axis_index(AXIS)
    group_barrier(n, me)

    def copy(a, k):
        p = lax.rem(me + k, n)
        return pltpu.make_async_remote_copy(srcs[a].at[p], dsts[a].at[me], ss.at[a, k], rs.at[a, k],
                                            device_id={AXIS: p}, device_id_type=MESH)

    for k in far_first(n):
        for a in range(arrays):
            copy(a, k).start()
    for k in far_first(n):
        for a in range(arrays):
            copy(a, k).wait()


def swap(n, cid, name, *arrays):
    m = len(arrays)
    return pl.pallas_call(
        functools.partial(swap_kernel, n, m),
        out_shape=tuple(jax.ShapeDtypeStruct(a.shape, a.dtype) for a in arrays),
        in_specs=[any_spec()] * m,
        out_specs=(any_spec(),) * m,
        scratch_shapes=[DMA((m, n)), DMA((m, n))],
        compiler_params=pltpu.CompilerParams(collective_id=cid, has_side_effects=True, vmem_limit_bytes=63 << 20),
        name=name,
    )(*arrays)


def swap_first_kernel(n, others, tc, spots, sent, need, do_hbm, *refs):
    pieces, refs = refs[:len(spots)], refs[len(spots):]
    (got, most, dh_hbm, dot_hbm, w_hbm, do_v, w_v, dot_v, dh_v, peers, relay,
     ss, rs, ns, nr, xs_sem, xr_sem, in_sem, w_sem, dh_sem, dot_sem, ms, mr, wo_sem) = refs
    me = lax.axis_index(AXIS)
    t, d = do_v.shape
    chips, fs = w_v.shape[1], w_v.shape[2] // 2
    nc = t // tc
    rows = lambda c: pl.ds(pl.multiple_of(c * tc, tc), tc)
    hops = []
    for name, size in others:
        reach = 1
        while reach < size:
            hops.append((name, size, reach))
            reach *= 2

    def piece(i):
        rel, row = spots[i]
        size = pieces[i].shape[0]
        return pltpu.make_async_copy(pieces[i], w_v.at[0, rel, pl.ds(row, size)], w_sem.at[i])

    def mate_copy(rel):
        return pltpu.make_async_remote_copy(w_v.at[0, rel], w_v.at[1, rel], ms.at[rel], mr.at[rel],
                                            device_id={AXIS: me + 1 - 2 * lax.rem(me, 2)}, device_id_type=MESH)

    def load(c):
        return pltpu.make_async_copy(do_hbm.at[rows(c)], do_v.at[rows(c)], in_sem.at[c])

    for i in range(len(spots)):
        piece(i).start()
    for c in range(nc):
        load(c).start()
    sem = pltpu.get_barrier_semaphore()
    for k in range(1, n):
        pl.semaphore_signal(sem, inc=1, device_id={AXIS: lax.rem(me + k, n)}, device_id_type=MESH)
    for name, size, reach in hops:
        at = lax.axis_index(name)
        pl.semaphore_signal(sem, inc=1, device_id={name: lax.rem(at + size - reach, size)}, device_id_type=MESH)
    pl.semaphore_wait(sem, n - 1 + len(hops))

    def row_copy(k):
        p = lax.rem(me + k, n)
        return pltpu.make_async_remote_copy(sent.at[p], got.at[me], ss.at[k], rs.at[k],
                                            device_id={AXIS: p}, device_id_type=MESH)

    def need_copy(k):
        return pltpu.make_async_remote_copy(need, peers.at[k], ns.at[k], nr.at[k],
                                            device_id={AXIS: lax.rem(me + k, n)}, device_id_type=MESH)

    for k in far_first(n):
        need_copy(k).start()
    for k in far_first(n):
        row_copy(k).start()
    for i in range(len(spots)):
        piece(i).wait()
    for rel in range(chips):
        mate_copy(rel).start()
    kept = pltpu.make_async_copy(w_v.at[0], w_hbm.at[0], wo_sem.at[0])
    kept.start()
    taken = pltpu.make_async_copy(w_v.at[1], w_hbm.at[1], wo_sem.at[1])

    def put(i):
        return pltpu.make_async_copy(dh_v.at[lax.rem(i, 2)], dh_hbm.at[lax.div(i, nc), rows(lax.rem(i, nc))],
                                     dh_sem.at[lax.rem(i, 2)])

    def body(i, carry):
        s, c = lax.div(i, nc), lax.rem(i, nc)

        @pl.when(i == nc * chips)
        def _():
            for rel in range(chips):
                mate_copy(rel).wait_recv()
            taken.start()

        @pl.when(s == 0)
        def _():
            load(c).wait()
            dot_v[:, rows(c)] = do_v[rows(c), :].T

        @pl.when(i >= 2)
        def _():
            put(i - 2).wait()

        dh_v[lax.rem(i, 2)] = dot_nt(do_v[rows(c), :], w_v[lax.div(s, chips), lax.rem(s, chips), pl.ds(fs, fs), :])
        put(i).start()
        return carry

    steps = n * nc
    lax.fori_loop(0, steps, body, 0)
    turned = pltpu.make_async_copy(dot_v, dot_hbm, dot_sem)
    turned.start()
    top = need[...]
    for k in range(1, n):
        need_copy(k).wait_recv()
        top = jnp.maximum(top, peers[k])
    for i, (name, size, reach) in enumerate(hops):
        relay[2 * i] = top
        at = lax.axis_index(name)
        hop = pltpu.make_async_remote_copy(relay.at[2 * i], relay.at[2 * i + 1], xs_sem.at[i], xr_sem.at[i],
                                           device_id={name: lax.rem(at + reach, size)}, device_id_type=MESH)
        hop.start()
        hop.wait()
        top = jnp.maximum(top, relay[2 * i + 1])
    most[...] = top
    for i in range(steps - 2, steps):
        put(i).wait()
    turned.wait()
    kept.wait()
    taken.wait()
    for rel in range(chips):
        mate_copy(rel).wait_send()
    for k in far_first(n):
        need_copy(k).wait_send()
        row_copy(k).wait()


def swap_first(n, others, sent, need, dout, pieces, spots, tc=1024):
    t, d = dout.shape
    fs = pieces[0].shape[0] // 2
    chips = n // 2
    nc = t // tc
    hops = max(1, sum((size - 1).bit_length() for _, size in others))
    tile = (8, LANES)
    w_shape = (2, chips, 2 * fs, d)
    return pl.pallas_call(
        functools.partial(swap_first_kernel, n, others, tc, spots),
        out_shape=(jax.ShapeDtypeStruct(sent.shape, sent.dtype), jax.ShapeDtypeStruct(tile, I32),
                   jax.ShapeDtypeStruct((n, t, fs), F32), jax.ShapeDtypeStruct((d, t), BF16),
                   jax.ShapeDtypeStruct(w_shape, BF16)),
        in_specs=[any_spec(), vmem_spec(), any_spec()] + [any_spec()] * len(pieces),
        out_specs=(any_spec(), vmem_spec(), any_spec(), any_spec(), any_spec()),
        scratch_shapes=[
            pltpu.VMEM((t, d), BF16), pltpu.VMEM(w_shape, BF16), pltpu.VMEM((d, t), BF16), pltpu.VMEM((2, tc, fs), F32),
            pltpu.VMEM((n,) + tile, I32), pltpu.VMEM((2 * hops,) + tile, I32),
            DMA((n,)), DMA((n,)), DMA((n,)), DMA((n,)), DMA((hops,)), DMA((hops,)), DMA((nc,)), DMA((len(pieces),)),
            DMA((2,)), DMA, DMA((chips,)), DMA((chips,)), DMA((2,)),
        ],
        compiler_params=pltpu.CompilerParams(collective_id=5, has_side_effects=True, vmem_limit_bytes=63 << 20),
        name='swap_first',
    )(sent, need, dout, *pieces)


def gather_weights(n, w_up_l, w_down_l):
    chips = n // 2
    fs = w_down_l.shape[0]
    ahead = [(i, (i + 2) % n) for i in range(n)]
    back = [(i, (i - 2) % n) for i in range(n)]
    own = jnp.concatenate([w_up_l.T, w_down_l], axis=0)
    pieces, spots = [own], [(0, 0)]
    behind = before = own
    for k in range(1, (chips - 1) // 2 + 1):
        behind = lax.ppermute(behind, AXIS, ahead)
        before = lax.ppermute(before, AXIS, back)
        pieces += [behind, before]
        spots += [(chips - k, 0), (k, 0)]
    return tuple(pieces), tuple(spots)


def expand_kernel(n, c, again, *refs):
    if again:
        who_ref, toks_h, lines_h, sent, got, x_prev, out, toks, lines, rb, rf, xg, x_out, i_sem, in_sem, o_sem, x_sem = refs
    else:
        who_ref, toks_h, lines_h, sent, got, out, toks, lines, rb, rf, xg, x_out, i_sem, in_sem, o_sem = refs
    me = who_ref[0]
    t, d = x_out.shape
    w = d // LANES
    idx = (pltpu.make_async_copy(toks_h, toks, i_sem.at[0]), pltpu.make_async_copy(lines_h, lines, i_sem.at[1]))
    for cp in idx:
        cp.start()
    own = pltpu.make_async_copy(sent.at[me], rb.at[me], in_sem.at[me])
    own.start()
    if again:
        prev = pltpu.make_async_copy(x_prev, x_out, x_sem)
        prev.start()

    def load(q):
        return pltpu.make_async_copy(got.at[q], rb.at[q], in_sem.at[q])

    for k in range(n):
        @pl.when(k != me)
        def _():
            load(k).start()
    if again:
        prev.wait()
        split_rows(x_out, xg, 0, t)

    def source(q, carry):
        load(q).wait()
        split_rows(rb.at[q], rf, q * c, c)
        return carry

    lax.fori_loop(0, n, source, 0)

    for cp in idx:
        cp.wait()

    def body(b, carry):
        vals = [rf[pl.ds(pl.multiple_of(lines[b * UNROLL + u], w), w), :] for u in range(UNROLL)]
        for u in range(UNROLL):
            xg[pl.ds(pl.multiple_of(toks[b * UNROLL + u], w), w), :] = vals[u]
        return carry

    lax.fori_loop(0, t // UNROLL, body, 0)
    step = t // 4
    for i in range(4):
        join_rows(xg.at[pl.ds(i * step * w, step * w)], x_out, i * step, step)
        part = pl.ds(i * step, step)
        pltpu.make_async_copy(x_out.at[part], out.at[part], o_sem).start()
    pltpu.make_async_copy(x_out, out, o_sem).wait()


def expand(n, rnd, who, toks, lines, sent, got, x_prev=None):
    again = x_prev is not None
    t = toks.shape[0]
    _, c, d = sent.shape
    w = d // LANES
    lines = lines - rnd[0] * (n * c * w)
    here = (lines >= 0) & (lines < n * c * w)
    toks, lines = jnp.where(here, toks, t * w), jnp.where(here, lines, 0)
    return pl.pallas_call(
        functools.partial(expand_kernel, n, c, again),
        out_shape=jax.ShapeDtypeStruct((t, d), BF16),
        in_specs=[smem_spec()] + [any_spec()] * (5 if again else 4),
        out_specs=any_spec(),
        scratch_shapes=[pltpu.SMEM((t,), I32), pltpu.SMEM((t,), I32),
                        pltpu.VMEM((n, c, d), BF16), pltpu.VMEM((n * c * w, LANES), F32),
                        pltpu.VMEM((t * w + 8, LANES), F32), pltpu.VMEM((t, d), BF16), DMA((2,)), DMA((n,)), DMA] + ([DMA] if again else []),
        compiler_params=pltpu.CompilerParams(vmem_limit_bytes=63 << 20),
        name='expand_more' if again else 'expand_rows',
    )(who, toks, lines, sent, got, *((x_prev,) if again else ()))


def collect_kernel(n, c1, c2, vocab, again, *refs):
    if again:
        rnd_ref, pack_h, toks_h, ids, dx_hbm, one_out, many_out, *rest = refs
    else:
        rnd_ref, pack_h, toks_h, ids, dx_hbm, y_in, up_in, down_in, one_out, many_out, y_out, up_out, down_out, *rest = refs
        *rest, y_v, up_v, down_v, side_v, side_sem = rest
    pack, toks, dx_v, dxf, g, col, one, many, i_sem, in_sem, o_sem = rest
    rnd = rnd_ref[0]
    t, d = dx_v.shape
    w = d // LANES
    parts = in_sem.shape[0]
    step = t // parts
    head = pack.shape[0] - PAGE
    last = head - c1 - c2

    def load(i):
        rows = pl.ds(pl.multiple_of(i * step, step), step)
        return pltpu.make_async_copy(dx_hbm.at[rows], dx_v.at[rows], in_sem.at[i])

    idx = (pltpu.make_async_copy(pack_h, pack, i_sem.at[0]), pltpu.make_async_copy(toks_h, toks, i_sem.at[1]))
    for cp in idx:
        cp.start()
    for i in range(parts):
        load(i).start()
    if not again:
        side_in = (pltpu.make_async_copy(y_in, y_v, side_sem.at[0]), pltpu.make_async_copy(up_in, up_v, side_sem.at[1]),
                   pltpu.make_async_copy(down_in, down_v, side_sem.at[2]))
        side_out = (pltpu.make_async_copy(y_v, y_out, side_sem.at[0]), pltpu.make_async_copy(up_v, up_out, side_sem.at[1]),
                    pltpu.make_async_copy(side_v, down_out, side_sem.at[2]))
        for cp in side_in:
            cp.start()
    for cp in idx:
        cp.wait()

    def name_rows(q, carry):
        at = jnp.minimum(pack[head + 16 + q] + rnd * c2, last)
        for j in range(c2):
            col[pl.ds(q * c2 + j, 1), :] = jnp.full((1, LANES), pack[at + j] + q * (vocab * w), I32)
        return carry

    lax.fori_loop(0, n, name_rows, 0)
    many[...] = jnp.zeros(many.shape, F32)
    names = col[:, :1]

    def sum_many(i, carry):
        load(i).wait()
        hot = jnp.where(names == ids[i] * w, 1.0, 0.0).astype(BF16)
        rows = pl.ds(pl.multiple_of(i * step, step), step)
        many[...] += lax.dot_general(hot, dx_v[rows, :], (((1,), (0,)), ((), ())), preferred_element_type=F32)
        split_rows(dx_v.at[rows], dxf, i * step, step)
        return carry

    lax.fori_loop(0, parts, sum_many, 0)
    pltpu.make_async_copy(many, many_out, o_sem.at[1]).start()
    if not again:
        for cp in side_in:
            cp.wait()
        side_v[...] = down_v[...].T
        for cp in side_out:
            cp.start()

    def owner(q, carry):
        at = jnp.minimum(pack[head + q] + rnd * c1, last)
        pick_rows(dxf, g, 0, c1, w, lambda j: toks[at + j])
        join_rows(g, one.at[q], 0, c1)
        pltpu.make_async_copy(one.at[q], one_out.at[q], o_sem.at[0]).start()
        return carry

    lax.fori_loop(0, n, owner, 0)
    pltpu.make_async_copy(one, one_out, o_sem.at[0]).wait()
    pltpu.make_async_copy(many, many_out, o_sem.at[1]).wait()
    if not again:
        for cp in side_out:
            cp.wait()


def collect(n, c1, c2, vocab, rnd, pack, toks, ids, dx, side=None):
    again = side is None
    t, d = dx.shape
    w = d // LANES
    parts = ids.shape[0]
    shapes = (jax.ShapeDtypeStruct((n, c1, d), BF16), jax.ShapeDtypeStruct((n * c2, d), F32))
    extra = []
    if not again:
        y, up, down = side
        shapes += (jax.ShapeDtypeStruct(y.shape, y.dtype), jax.ShapeDtypeStruct(up.shape, F32),
                   jax.ShapeDtypeStruct(down.shape[::-1], F32))
        extra = [pltpu.VMEM(y.shape, y.dtype), pltpu.VMEM(up.shape, F32), pltpu.VMEM(down.shape, F32),
                 pltpu.VMEM(down.shape[::-1], F32), DMA((3,))]
    one, many, *rest = pl.pallas_call(
        functools.partial(collect_kernel, n, c1, c2, vocab, again),
        out_shape=shapes,
        in_specs=[smem_spec(), any_spec(), any_spec(), vmem_spec(), any_spec()] + [any_spec()] * (0 if again else 3),
        out_specs=(any_spec(),) * len(shapes),
        scratch_shapes=[pltpu.SMEM(pack.shape, I32), pltpu.SMEM(toks.shape, I32),
                        pltpu.VMEM((t, d), BF16), pltpu.VMEM((t * w, LANES), F32), pltpu.VMEM((c1 * w, LANES), F32),
                        pltpu.VMEM((n * c2, LANES), I32), pltpu.VMEM((n, c1, d), BF16), pltpu.VMEM((n * c2, d), F32),
                        DMA((2,)), DMA((parts,)), DMA((2,))] + extra,
        compiler_params=pltpu.CompilerParams(vmem_limit_bytes=63 << 20),
        name='collect_more' if again else 'collect_rows',
    )(rnd, pack, toks, ids, dx, *(() if again else side))
    return (one, many.reshape(n, c2, d)) + tuple(rest)


def place_kernel(n, c1, c2, again, *refs):
    if again:
        rnd_ref, who_ref, lists, one_own, many_own, one, many, _, out, ls, acc, o_v, m_v, f_v, st, l_sem, in_sem, out_sem = refs
    else:
        rnd_ref, who_ref, lists, one_own, many_own, one, many, out, ls, acc, o_v, m_v, f_v, st, l_sem, in_sem, out_sem = refs
    me, rnd = who_ref[0], rnd_ref[0]
    vocab, d = out.shape
    w = d // LANES
    asked = pltpu.make_async_copy(lists, ls, l_sem)
    asked.start()
    pl_len = ls.shape[0] // n
    head = pl_len - PAGE

    def load(q):
        return (pltpu.make_async_copy(one.at[q], o_v.at[q], in_sem.at[0, q]),
                pltpu.make_async_copy(many.at[q], m_v.at[q], in_sem.at[1, q]))

    pltpu.make_async_copy(one_own.at[me], o_v.at[me], in_sem.at[0, me]).start()
    pltpu.make_async_copy(many_own.at[me], m_v.at[me], in_sem.at[1, me]).start()
    for k in range(n):
        @pl.when(k != me)
        def _():
            for part in load(k):
                part.start()
    blk = st.shape[1]

    def span(i):
        return pl.ds(pl.multiple_of(i * blk, blk), blk)

    def split8(src, row):
        def one8(r0):
            for k in range(w):
                acc[pl.ds((row + r0) * w + k, 8, stride=w), :] = src[pl.ds(r0, 8), pl.ds(k * LANES, LANES)]
        blocks(blk, 8, 8, one8)

    if again:
        def bring(i, carry):
            pltpu.make_async_copy(out.at[span(i)], st.at[0], out_sem.at[0]).start()
            pltpu.make_async_copy(out.at[span(i)], st.at[0], out_sem.at[0]).wait()
            split8(st.at[0], i * blk)
            return carry

        lax.fori_loop(0, vocab // blk, bring, 0)
    else:
        zero = jnp.zeros((16 * w, LANES), F32)

        def clear(r0):
            acc[pl.ds(r0 * w, 16 * w), :] = zero

        blocks(vocab, 16, 4, clear)
    asked.wait()
    dump = vocab * w

    def add(count, at, row0):
        def body(b, carry):
            lines, sums = [], []
            for u in range(UNROLL_ADD):
                j = b * UNROLL_ADD + u
                line = pl.multiple_of(jnp.where(j < count, ls[at + j], dump), w)
                lines.append(line)
                src = f_v[pl.ds(pl.multiple_of((row0 + j) * w, w), w), :]
                sums.append(acc[pl.ds(line, w), :] + src)
            for u in range(UNROLL_ADD):
                acc[pl.ds(lines[u], w), :] = sums[u]
            return carry

        lax.fori_loop(0, lax.div(count + UNROLL_ADD - 1, UNROLL_ADD), body, 0)

    def source(q, carry):
        for part in load(q):
            part.wait()
        at = q * pl_len + head
        split_rows(o_v.at[q], f_v, 0, c1)
        split_rows(m_v.at[q], f_v, c1, c2)
        b1, b2 = ls[at + me] + rnd * c1, ls[at + 16 + me] + rnd * c2
        e1, e2 = ls[at + me + 1], ls[at + 16 + me + 1]
        add(jnp.clip(e1 - b1, 0, c1), q * pl_len + b1, 0)
        add(jnp.clip(e2 - b2, 0, c2), q * pl_len + b2, c1)
        return carry

    lax.fori_loop(0, n, source, 0)

    def emit(i, carry):
        slot = lax.rem(i, 2)

        @pl.when(i >= 2)
        def _():
            pltpu.make_async_copy(st.at[slot], out.at[span(i - 2)], out_sem.at[slot]).wait()

        def one8(r0):
            for k in range(w):
                st[slot, pl.ds(r0, 8), pl.ds(k * LANES, LANES)] = acc[pl.ds((i * blk + r0) * w + k, 8, stride=w), :]

        blocks(blk, 8, 8, one8)
        pltpu.make_async_copy(st.at[slot], out.at[span(i)], out_sem.at[slot]).start()
        return carry

    total = vocab // blk
    lax.fori_loop(0, total, emit, 0)
    for i in range(max(0, total - 2), total):
        pltpu.make_async_copy(st.at[i % 2], out.at[span(i)], out_sem.at[i % 2]).wait()


def place(n, c1, c2, vocab, rnd, who, lists, one_own, many_own, one, many, prev=None):
    again = prev is not None
    d = one.shape[-1]
    w = d // LANES
    blk = next(b for b in range(1280, 0, -8) if vocab % b == 0)
    return pl.pallas_call(
        functools.partial(place_kernel, n, c1, c2, again),
        out_shape=jax.ShapeDtypeStruct((vocab, d), F32),
        in_specs=[smem_spec()] * 2 + [any_spec()] * (6 if again else 5),
        out_specs=any_spec(),
        scratch_shapes=[
            pltpu.SMEM(lists.shape, I32), pltpu.VMEM((vocab * w + 8, LANES), F32), pltpu.VMEM((n, c1, d), BF16), pltpu.VMEM((n, c2, d), F32),
            pltpu.VMEM(((c1 + c2) * w, LANES), F32), pltpu.VMEM((2, blk, d), F32), DMA, DMA((2, n)), DMA((2,)),
        ],
        input_output_aliases={7: 0} if again else {},
        compiler_params=pltpu.CompilerParams(vmem_limit_bytes=63 << 20),
        name='place_more' if again else 'place_rows',
    )(rnd, who, lists, one_own, many_own, one, many, *((prev,) if again else ()))


def route(n, vocab, w, c1, c2, ids):
    t = ids.shape[0]
    c = c1 + c2
    s, p = lax.sort((ids, lax.iota(I32, t)), num_keys=1)
    edge = jnp.full((1,), -1, I32)
    first = s != jnp.concatenate([edge, s[:-1]])
    last = s != jnp.concatenate([s[1:], edge])
    lone = first & last
    lead = first & ~last
    lone_i, lead_i = lone.astype(I32), lead.astype(I32)
    bounds = lax.iota(I32, n + 1) * vocab
    below = s[None, :] < bounds[:, None]
    base1 = jnp.sum(jnp.where(below, lone_i[None, :], 0), axis=1)
    base2 = jnp.sum(jnp.where(below, lead_i[None, :], 0), axis=1)
    owner = n - jnp.sum(below[1:].astype(I32), axis=0)
    mine = owner[None, :] == lax.iota(I32, n)[:, None]
    start1 = jnp.sum(jnp.where(mine, base1[:n, None], 0), axis=0)
    start2 = jnp.sum(jnp.where(mine, base2[:n, None], 0), axis=0)
    r1 = jnp.cumsum(lone_i) - lone_i - start1
    r2 = jnp.cumsum(lead_i) - 1 - start2
    rnd1, rnd2 = r1 // c1, r2 // c2
    slot = jnp.where(lone, rnd1 * (n * c) + owner * c + r1 - rnd1 * c1, rnd2 * (n * c) + owner * c + c1 + r2 - rnd2 * c2)
    kind = jnp.where(lone, 0, jnp.where(lead, 1, 2)) * t + lax.iota(I32, t)
    _, line, tok = lax.sort((kind, (s - owner * vocab) * w, p * w), num_keys=1)
    n1 = base1[n]
    room = -(-(t + c1 + c2) // PAGE) * PAGE
    spare = jnp.zeros((16 - n - 1,), I32)
    heads = jnp.concatenate([base1, spare, n1 + base2, spare])
    fill = jnp.zeros((room - t,), I32)
    heads = jnp.concatenate([heads, jnp.zeros((PAGE - heads.shape[0],), I32)])
    pack = jnp.concatenate([line, fill, heads])
    lone_tok = jnp.concatenate([tok, fill])
    per1 = jnp.max(base1[1:] - base1[:-1])
    per2 = jnp.max(base2[1:] - base2[:-1])
    rounds = jnp.maximum((per1 + c1 - 1) // c1, (per2 + c2 - 1) // c2)
    return pack, lone_tok, p * w, slot * w, rounds


def solution(mesh):
    n = mesh.shape[AXIS]
    axes = tuple(mesh.axis_names)
    others = tuple((name, mesh.shape[name]) for name in axes if name != AXIS)
    tok_spec = P(axes)
    row_spec = P(axes, None)

    def local_step(token_ids, emb_shard, norm_gain, w_up_l, w_down_l, grad_out):
        vocab, d = emb_shard.shape
        t = token_ids.shape[0]
        w = d // LANES
        c1 = -(-(t * 5 // (8 * n)) // 16) * 16
        c2 = -(-(t // 128) // 16) * 16
        who = lax.axis_index(AXIS)[None].astype(I32)
        pieces, spots = gather_weights(n, w_up_l, w_down_l)
        pack, lone_tok, toks, lines, rounds = route(n, vocab, w, c1, c2, token_ids)
        lists, across = share(n, pack, pieces[-2], pieces[-1])
        if n % 4 == 0:
            pieces, spots = pieces + (across,), spots + ((n // 4, 0),)
        none = jnp.zeros((1,), I32)

        def rows_of(rnd):
            sent = serve(n, c1, c2, rnd, who, lists, emb_shard)
            return sent, swap(n, 2, 'swap_rows', sent)[0]

        def more_rows(carry):
            r, x_now = carry
            return r + 1, expand(n, r[None], who, toks, lines, *rows_of(r[None]), x_now)

        sent = serve(n, c1, c2, none, who, lists, emb_shard)
        got, most, dh, dot, ws = swap_first(n, others, sent, jnp.full((8, LANES), rounds, I32), grad_out, pieces, spots)
        rounds = most[0, 0]
        x = expand(n, none, who, toks, lines, sent, got)
        _, x = lax.while_loop(lambda carry: carry[0] < rounds, more_rows, (jnp.ones((), I32), x))
        out, dx, dw1, dw2t = mlp(n, 4, x, norm_gain, ws, grad_out, dh, dot)
        ids_c = token_ids.reshape(-1, 1, t // 8)

        one, many, out, dw1, dw2 = collect(n, c1, c2, vocab, none, pack, lone_tok, ids_c, dx, (out, dw1, dw2t))

        def more_sums(carry):
            r, now = carry
            mine = collect(n, c1, c2, vocab, r[None], pack, lone_tok, ids_c, dx)
            return r + 1, place(n, c1, c2, vocab, r[None], who, lists, *mine, *swap(n, 3, 'swap_sums', *mine), now)

        d_emb = place(n, c1, c2, vocab, none, who, lists, one, many, *swap(n, 3, 'swap_sums', one, many))
        _, d_emb = lax.while_loop(lambda carry: carry[0] < rounds, more_sums, (jnp.ones((), I32), d_emb))
        return out, d_emb, dw1, dw2

    return jax.shard_map(
        local_step,
        mesh=mesh,
        in_specs=(tok_spec, P(AXIS, None), P(None), P(None, AXIS), P(AXIS, None), row_spec),
        out_specs=(row_spec, row_spec, P(axes[0], AXIS), row_spec),
        check_vma=False,
    )
```
